32 devices in a mesh: wide: 16 (over z, y, core), narrow: 2 (over x).
Axes of the slice: x: 2, y: 2, z: 4, core: 2. Of those that a mesh axis runs over, the one named last changes fastest.
Arguments:
- src_field: bfloat16 [2, 16, 65536], P(None, 'narrow', 'wide'), may hold values from -6 to 6
- src_depth: int32 [65536], P(('wide', 'narrow')), may hold values from 0 to 16, as said below
- packed_counts: int32 [4096, 64, 128], P(('wide', 'narrow')), may hold values from 0 to 100664832, as said below
- pair_source: int32 [4096], P(('wide', 'narrow')), may hold values from 0 to 15
- pair_home: int32 [4096], P(('wide', 'narrow')), may hold values from 0 to 1023, as said below
- pair_count: int32 [32], P(('wide', 'narrow')), may hold values from 64 to 128, as said below
Outputs:
- remapped: bfloat16 [2, 16, 131072], P(None, 'narrow', 'wide')
The draws below stay inside these ranges and needn't reach their ends.
Inputs may be any that keep to these rules, and one draw needn't show every extreme that they name: `src_depth`: depth 0 marks a dry source cell. `packed_counts`: word (p, i, j) holds count (p, i, j) plus 65536 times count (p, i + 64, j); every count lies between 0 and 1536. The target block pair_home[p] is held by wide index pair_home[p] // 64, which differs by at most 2, counted cyclically over the wide axis, from the wide index of the device that holds pair p. Among the 128 pairs of one device at most 51 have target blocks on one wide index, and on some wide index exactly 51 live pairs of that device. A device's pairs from position pair_count[d] on are padding; some device has all 128 live.
All inputs are finite; a program needn't handle non-finite values.
Results may differ from the reference program's by a relative error of at most 0.0054.
Values may be sent and summed in bfloat16 or wider, within the bound.
A program may use at most 64 MiB of HBM per device.

```python
import jax
import jax.numpy as jnp
from jax import lax

BLK = 128
LEV = 16
VARS = 2
DENOM = 256
REACH = 2
SB_DEV = 16
P_DEV = 128
TB_DEV = 64
CAP = 51
PAIRS = 4096
SRC_CELLS = 65536
N_WIDE = 16
N_NARROW = 2


def draw_src_depth(key, part):
    key = jax.random.fold_in(key, 404)
    key_land, key_depth = jax.random.split(key)
    blocks = SB_DEV * N_WIDE * N_NARROW
    sea_mask = (jax.random.randint(key_land, (blocks, 1), 0, 5) >= 3).astype(jnp.int32)
    cell_depth = jax.random.randint(key_depth, (blocks, BLK), 1, LEV + 1)
    return (cell_depth * sea_mask).reshape(blocks * BLK).astype(jnp.int32)


def draw_packed_counts(key, part):
    key = jax.random.fold_in(key, 101)
    half_rows = BLK // 2
    key_list = jax.random.split(key, 6)
    array_shape = (P_DEV * N_WIDE * N_NARROW, half_rows, BLK)
    row_ids = jnp.arange(half_rows, dtype=jnp.int32)[:, None]
    column_ids = jnp.arange(BLK, dtype=jnp.int32)[None, :]

    def half_counts(key_spread, key_power, key_factor, offset):
        spread = jax.random.randint(key_spread, array_shape, 0, 4)
        exponent = jax.random.randint(key_power, (array_shape[0], half_rows, 1), 0, 10)
        factor = jax.random.randint(key_factor, (array_shape[0], half_rows, 1), 1, 4)
        diagonal = jnp.power(2, exponent) * factor
        on_diagonal = (column_ids == row_ids + offset)[None, :, :]
        return jnp.where(on_diagonal, diagonal, spread)
    lower_half = half_counts(key_list[0], key_list[1], key_list[2], 0)
    upper_half = half_counts(key_list[3], key_list[4], key_list[5], half_rows)
    return (lower_half + 65536 * upper_half).astype(jnp.int32)


def draw_pair_home(key, part):
    key = jax.random.fold_in(key, 202)
    devices = N_WIDE * N_NARROW
    offset_total = 2 * REACH + 1
    key_rows, key_place = jax.random.split(key)
    head_rows = P_DEV // 2
    slot_ids = jnp.arange(offset_total * CAP, dtype=jnp.int32) // CAP
    wide_of = jnp.arange(devices, dtype=jnp.int32) // N_NARROW

    def one_device(row_key, wide_index):
        key_order, key_head, key_tail = jax.random.split(row_key, 3)
        offset_order = jax.random.permutation(key_order, offset_total).astype(jnp.int32)
        wanted = offset_order[slot_ids][:P_DEV]
        ordering = jnp.concatenate([jax.random.permutation(key_head, head_rows), head_rows + jax.random.permutation(key_tail, P_DEV - head_rows)])
        chosen = wanted[ordering]
        return (wide_index + chosen - REACH + N_WIDE) % N_WIDE
    owners = jax.vmap(one_device)(jax.random.split(key_rows, devices), wide_of)
    local_block = jax.random.randint(key_place, (devices, P_DEV), 0, TB_DEV)
    return (owners * TB_DEV + local_block).reshape(devices * P_DEV).astype(jnp.int32)


def draw_pair_count(key, part):
    key = jax.random.fold_in(key, 303)
    devices = N_WIDE * N_NARROW
    key_counts, key_full = jax.random.split(key)
    counts = jax.random.randint(key_counts, (devices,), P_DEV // 2, P_DEV + 1)
    fullest = jax.random.randint(key_full, (), 0, devices)
    return counts.at[fullest].set(P_DEV).astype(jnp.int32)


def with_ends(result, stream_key, low, high):
    dims = result.shape
    place = [jax.random.randint(jax.random.fold_in(stream_key, axis), (), 0, dims[axis]) for axis in range(len(dims))]
    result = result.at[tuple(place)].set(low)
    longest = dims.index(max(dims))
    place[longest] = (place[longest] + 1) % dims[longest]
    return result.at[tuple(place)].set(high)


def shard_levels(key, extent, cuts, smallest, high):
    def one(position, blocks):
        heights = jax.random.uniform(jax.random.fold_in(jax.random.fold_in(key, 6), position), (blocks,), jnp.float32, smallest / len(cuts), high / len(cuts))
        return jnp.repeat(jnp.exp(heights), extent[position] // blocks).reshape((-1,) + (1,) * (len(extent) - position - 1))

    loudness = one(*cuts[0])
    for cut in cuts[1:]:
        loudness = loudness * one(*cut)
    return loudness


def noise(stream_key, dims, width, most, cuts=(), kind=jnp.bfloat16):
    level = shard_levels(stream_key, dims, cuts, -0.22, 0.18) if cuts else 1.0
    drawn = jax.random.normal(stream_key, dims, jnp.float32) * width * level
    return jnp.minimum(jnp.maximum(drawn, -most), most).astype(kind)


def setup_inputs(seed: int = 0) -> dict:
    streams_of = jax.random.split(jax.random.key(seed), 7)
    src_field = noise(streams_of[0], (VARS, LEV, SRC_CELLS), 1.0, 6.0, ((1, 2), (2, 16)))
    src_depth = draw_src_depth(jax.random.fold_in(streams_of[6], 71), 0)
    packed_counts = draw_packed_counts(jax.random.fold_in(streams_of[6], 71), 0)
    pair_source = with_ends(jax.random.randint(streams_of[3], (PAIRS,), 0, SB_DEV), jax.random.fold_in(streams_of[3], 1), 0, SB_DEV - 1).astype(jnp.int32)
    pair_home = draw_pair_home(jax.random.fold_in(streams_of[6], 71), 0)
    pair_count = draw_pair_count(jax.random.fold_in(streams_of[6], 71), 0)
    return dict(src_field=src_field, src_depth=src_depth, packed_counts=packed_counts, pair_source=pair_source, pair_home=pair_home, pair_count=pair_count)


wet_limit = 1e-3


def unpack_counts(packed_words):
    lower_half = packed_words % 65536
    upper_half = packed_words // 65536
    return jnp.concatenate([lower_half, upper_half], axis=-2)


def stack_cells(field_block, depth_cells):
    level_ids = jnp.arange(field_block.shape[1], dtype=jnp.int32)
    wet_levels = level_ids[:, None] < depth_cells[None, :]
    masked = jnp.where(wet_levels[None, :, :], field_block, jnp.zeros_like(field_block))
    wet_ones = wet_levels.astype(field_block.dtype)
    return jnp.concatenate([jnp.transpose(masked, (1, 0, 2)), wet_ones[:, None, :]], axis=1)


def reference(src_field, src_depth, packed_counts, pair_source, pair_home, pair_count):
    device_total = pair_count.shape[0]
    own_cells = SB_DEV * BLK
    components = VARS + 1
    block_total = jnp.zeros((TB_DEV * N_WIDE, LEV, components, BLK), jnp.float32)

    def add_device(device_index, running):
        device_index = device_index.astype(jnp.int32)
        device_field = lax.dynamic_slice_in_dim(src_field, device_index * own_cells, own_cells, 2)
        cell_depth = lax.dynamic_slice_in_dim(src_depth, device_index * own_cells, own_cells, 0)
        device_packed = lax.dynamic_slice_in_dim(packed_counts, device_index * P_DEV, P_DEV, 0)
        source = lax.dynamic_slice_in_dim(pair_source, device_index * P_DEV, P_DEV, 0)
        home_block = lax.dynamic_slice_in_dim(pair_home, device_index * P_DEV, P_DEV, 0)
        live_count = lax.dynamic_slice_in_dim(pair_count, device_index, 1, 0)[0]
        stacked = stack_cells(device_field, cell_depth).reshape(LEV, components, SB_DEV, BLK)
        picked = jnp.take(stacked, source, axis=2)
        weight = (unpack_counts(device_packed).astype(jnp.float32) / DENOM).astype(jnp.bfloat16)
        pair_terms = jnp.einsum("pts,lcps->plct", weight.astype(jnp.float32), picked.astype(jnp.float32))
        pair_terms = lax.optimization_barrier(pair_terms.astype(jnp.bfloat16)).astype(jnp.float32)
        is_live = jnp.arange(P_DEV, dtype=jnp.int32) < live_count
        pair_terms = jnp.where(is_live[:, None, None, None], pair_terms, jnp.zeros_like(pair_terms))
        return running.at[home_block].add(pair_terms)

    block_total = lax.fori_loop(0, device_total, add_device, block_total)
    numerators = block_total[:, :, :VARS, :]
    wet_total = block_total[:, :, VARS, :]
    covered = wet_total > wet_limit
    safe_wet = jnp.where(covered, wet_total, jnp.ones_like(wet_total))
    remapped = jnp.where(covered[:, :, None, :], numerators / safe_wet[:, :, None, :], jnp.zeros_like(numerators))
    remapped = jnp.transpose(remapped, (2, 1, 0, 3)).reshape(VARS, LEV, TB_DEV * N_WIDE * BLK)
    return remapped.astype(jnp.bfloat16)
```

```python
import functools

import jax
import jax.numpy as jnp
from jax import lax
from jax.experimental import pallas as pl
from jax.experimental.pallas import tpu as pltpu
from jax.sharding import PartitionSpec as P

DENOM = 256
REACH = 2
TB_DEV = 64


wet_limit = 0.001


def passed_along(block, axis, distance):
    devices = range(lax.axis_size(axis))
    route = [((i - distance) % len(devices), i) for i in devices]
    return lax.ppermute(block, axis, route)


def unpack_counts(packed_words):
    return jnp.concatenate([packed_words % 65536, packed_words // 65536], axis=-2)


def block_sums(targets, received, block_count):
    owners = jnp.arange(block_count, dtype=jnp.int32)
    select = (targets[:, None] == owners[None, :]).astype(jnp.bfloat16)
    return jnp.einsum("rq,rlcb->lcqb", select, received, preferred_element_type=jnp.float32)


def by_collectives(src_field, src_depth, packed_counts, pair_source, pair_home, pair_count):
    narrow_size = lax.axis_size("narrow")
    wide_size = lax.axis_size("wide")
    field_vars = src_field.shape[0]
    components = field_vars + 1
    block_cells = packed_counts.shape[2]
    own_cells = src_depth.shape[0]
    own_tiles = own_cells // block_cells
    pair_slots = pair_source.shape[0]
    offset_count = 2 * REACH + 1
    capacity = max(2, 2 * pair_slots // offset_count)
    own_field = lax.all_to_all(src_field, "narrow", split_axis=2, concat_axis=1, tiled=True)
    levels = own_field.shape[1]
    part_levels = levels // narrow_size
    level_ids = jnp.arange(levels, dtype=jnp.int32)
    wet_levels = level_ids[:, None] < src_depth[None, :]
    masked = jnp.where(wet_levels[None, :, :], own_field, jnp.zeros_like(own_field))
    stacked = jnp.concatenate(
        [jnp.transpose(masked, (1, 0, 2)), wet_levels.astype(jnp.bfloat16)[:, None, :]], axis=1
    )
    by_tile = jnp.transpose(stacked.reshape(levels * components, own_tiles, block_cells), (1, 0, 2))
    picked = jnp.take(by_tile, pair_source, axis=0)
    weight = (unpack_counts(packed_counts).astype(jnp.float32) / DENOM).astype(jnp.bfloat16)
    pair_terms = lax.dot_general(
        picked, weight, (((2,), (2,)), ((0,), (0,))), preferred_element_type=jnp.float32
    )
    pair_terms = pair_terms.astype(jnp.bfloat16)
    is_live = jnp.arange(pair_slots, dtype=jnp.int32) < pair_count[0]
    wide_index = lax.axis_index("wide")
    destination = pair_home // TB_DEV
    local_block = pair_home % TB_DEV
    offset_index = (destination - wide_index + REACH + wide_size) % wide_size
    bound_for = (
        (offset_index[:, None] == jnp.arange(offset_count, dtype=jnp.int32)[None, :])
        & is_live[:, None]
    ).astype(jnp.int32)
    before = jnp.cumsum(bound_for, axis=0) - bound_for
    position = jnp.sum(before * bound_for, axis=1)
    slot_index = jnp.where(is_live, offset_index * capacity + position, offset_count * capacity)
    outgoing = (
        jnp.zeros((offset_count * capacity, levels * components, block_cells), jnp.bfloat16)
        .at[slot_index]
        .set(pair_terms, mode="drop")
    )
    targets = (
        jnp.full((offset_count * capacity,), TB_DEV, jnp.int32)
        .at[slot_index]
        .set(local_block, mode="drop")
    )
    outgoing = outgoing.reshape(offset_count, capacity, levels, components, block_cells)
    targets = targets.reshape(offset_count, capacity)
    shift_list = [shift_by for shift_by in range(-REACH, REACH + 1) if shift_by != 0]
    partial_value = block_sums(targets[REACH], outgoing[REACH], TB_DEV)
    for shift_by in shift_list:
        moved_terms, moved_owners = passed_along(
            (outgoing[REACH + shift_by], targets[REACH + shift_by]), "wide", shift_by
        )
        partial_value = partial_value + block_sums(moved_owners, moved_terms, TB_DEV)
    block_totals = lax.psum_scatter(partial_value, "narrow", scatter_dimension=0, tiled=True)
    numerators = block_totals[:, :field_vars]
    wet_total = block_totals[:, field_vars]
    covered = wet_total > wet_limit
    safe_wet = jnp.where(covered, wet_total, jnp.ones_like(wet_total))
    result = jnp.where(covered[:, None], numerators / safe_wet[:, None], jnp.zeros_like(numerators))
    result = jnp.transpose(result, (1, 0, 2, 3)).reshape(
        field_vars, part_levels, TB_DEV * block_cells
    )
    return result.astype(jnp.bfloat16)


SELF, MATE, RELAY, AHEAD, BEHIND = range(5)
LOADS = 4
EARLY = 3
SKEW = 8
VMEM_LIMIT = 67043328


def remap_kernel(
    sizes,
    field_hbm,
    depth_hbm,
    packed_hbm,
    source_hbm,
    home_hbm,
    count_hbm,
    out_ref,
    field,
    depth,
    source,
    home,
    count,
    field_in,
    slot_own,
    slot_in,
    words,
    weight,
    wets,
    fields_at,
    terms,
    cross_out,
    cross_in,
    own_terms,
    self_sum,
    sums_out,
    mate_in,
    ahead_in,
    behind_in,
    inverse,
    staged,
    ready,
    load_sems,
    small_sems,
    entry_sems,
    early_sems,
    cross_sems,
    mate_sems,
    ahead_sems,
    behind_sems,
):
    wide_size, fields, levels, tiles, cells, pairs = sizes
    planes = (fields + 1) * levels
    pitch = pairs + SKEW
    f32, bf16, i32 = jnp.float32, jnp.bfloat16, jnp.int32
    w = lax.axis_index("wide")
    n = lax.axis_index("narrow")
    other = 1 - n
    sign = 1 - 2 * lax.rem(w, 2)
    mate = w + sign
    ahead = lax.rem(w + 2 * sign + wide_size, wide_size)
    behind = lax.rem(w - 2 * sign + wide_size, wide_size)

    def signal(sem, place):
        pl.semaphore_signal(sem, inc=1, device_id=place, device_id_type=pl.DeviceIdType.MESH)

    barrier = pltpu.get_barrier_semaphore()
    signal(barrier, (w, other))
    signal(barrier, (mate, n))
    for far in (ahead, behind):

        @pl.when(far > w)
        def _():
            signal(barrier, (far, n))

    small = []
    for i, (src, dst) in enumerate(
        (
            (field_hbm, field),
            (depth_hbm, depth),
            (source_hbm, source),
            (home_hbm, home),
            (count_hbm, count),
        )
    ):
        load = pltpu.make_async_copy(src, dst, small_sems.at[i])
        load.start()
        small.append(load)
    per_load = pairs // LOADS
    loads = []
    for i in range(LOADS):
        span = pl.ds(i * per_load, per_load)
        load = pltpu.make_async_copy(packed_hbm.at[span], words.at[span], load_sems.at[i])
        load.start()
        loads.append(load)

    def remote(src, dst, sems, index, place):
        return pltpu.make_async_remote_copy(
            src_ref=src,
            dst_ref=dst,
            send_sem=sems.at[(0,) + index],
            recv_sem=sems.at[(1,) + index],
            device_id=place,
            device_id_type=pl.DeviceIdType.MESH,
        )

    own_cells = tiles * cells
    theirs = pl.ds(pl.multiple_of(other * own_cells, own_cells), own_cells)
    pl.semaphore_wait(barrier, 2 + (ahead < w).astype(i32) + (behind < w).astype(i32))
    for i, far in ((1, ahead), (0, behind)):

        @pl.when(far < w)
        def _():
            signal(ready.at[i], (far, n))

    small[0].wait()
    entry = [remote(field.at[:, :, theirs], field_in, entry_sems, (0,), (w, other))]
    entry[0].start()

    small[1].wait()
    rows = lax.broadcasted_iota(i32, (2 * levels, cells), 0)
    level_of = jnp.where(rows < levels, rows + other * levels, rows - levels + n * levels)
    for tile in range(tiles):
        wet = level_of < depth[pl.ds(tile, 1), :]
        wets[tile] = jnp.where(wet, 1.0, 0.0).astype(bf16)

    half = cells // 2

    def unpack(first):
        for u in range(per_load):
            p = first + u
            word = words[p]
            lanes = pl.ds((u % 2) * cells, cells)
            low = (word & 65535).astype(f32).astype(bf16)
            high = (word >> 16).astype(f32).astype(bf16)
            weight[(first + u) // 2, pl.ds(0, half), lanes] = low
            weight[(first + u) // 2, pl.ds(half, half), lanes] = high

    def multiply(values_of, count, base, first):
        zero = jnp.zeros((count, cells), bf16)
        for u in range(0, per_load, 2):
            p = first + u
            left = jnp.concatenate([values_of[source[p]], zero], axis=1)
            right = jnp.concatenate([zero, values_of[source[p + 1]]], axis=1)
            term = lax.dot_general(
                jnp.concatenate([left, right], axis=0),
                weight[p // 2],
                (((1,), (1,)), ((), ())),
                preferred_element_type=f32,
            )
            terms[pl.ds(base * pitch + p, count, stride=pitch), :] = term[:count]
            terms[pl.ds(base * pitch + p + 1, count, stride=pitch), :] = term[count:]

    def rounded(row, start, count):
        return terms[pl.ds(row * pitch + start, count), :].astype(bf16)

    small[2].wait()
    loads[0].wait()
    unpack(0)
    cross = [[] for _ in range(planes)]
    for batch in range(LOADS):
        first = batch * per_load
        if batch + 1 < LOADS:
            loads[batch + 1].wait()
            unpack(first + per_load)
        multiply(wets, 2 * levels, 0, first)
        span = pl.ds(first, per_load)
        for q in range(EARLY):
            cross_out[q, span, :] = rounded(q, first, per_load)
        some = pl.ds(0, EARLY)
        copy = remote(
            cross_out.at[some, span, :], cross_in.at[some, span, :],
            early_sems, (batch,), (w, other),
        )
        copy.start()
        cross[0].append(copy)

    def send_terms(q):
        cross_out[q] = rounded(q if q < levels else q + levels, 0, pairs)
        copy = remote(cross_out.at[q], cross_in.at[q], cross_sems, (q - EARLY,), (w, other))
        copy.start()
        cross[q].append(copy)

    for q in range(EARLY, levels):
        send_terms(q)

    small[3].wait()
    small[4].wait()
    wide_home = lax.div(home[...], TB_DEV)
    offset = lax.rem(wide_home - w + REACH + wide_size, wide_size) - REACH
    toward = offset * sign
    slot = jnp.where(toward > 0, 2 * toward - 1, -2 * toward)
    is_live = lax.broadcasted_iota(i32, (1, pairs), 1) < count[0]
    slot_own[...] = jnp.where(is_live, slot * TB_DEV + home[...] - wide_home * TB_DEV, -1)
    entry.append(remote(slot_own, slot_in, entry_sems, (1,), (w, other)))
    entry[1].start()

    level_ids = lax.broadcasted_iota(i32, (levels, cells), 0)

    def stack(side, group, read):
        for tile in range(tiles):
            wet = level_ids + group * levels < depth[pl.ds(tile, 1), :]
            values = [jnp.where(wet, read(k, tile).astype(f32), 0.0) for k in range(fields)]
            fields_at[tile, pl.ds(side * fields * levels, fields * levels), :] = (
                jnp.concatenate(values, axis=0).astype(bf16)
            )

    own_start = n * own_cells
    stack(
        1,
        n,
        lambda k, tile: field[k, :, pl.ds(pl.multiple_of(own_start + tile * cells, cells), cells)],
    )
    for q in range(levels):
        own_terms[q] = rounded(q + levels, 0, pairs)

    entry[0].wait()
    stack(0, other, lambda k, tile: field_in[k, :, pl.ds(tile * cells, cells)])

    def batch_of_fields(batch, carry):
        multiply(fields_at, 2 * fields * levels, 2 * levels, batch * per_load)
        return carry

    lax.fori_loop(0, LOADS, batch_of_fields, 0)
    for q in range(levels, planes):
        send_terms(q)
    for q in range(levels, planes):
        own_terms[q] = rounded(q + levels + fields * levels, 0, pairs)

    entry[1].wait()
    slots = lax.broadcasted_iota(i32, (5 * TB_DEV, pairs), 0)
    select = jnp.concatenate(
        [
            jnp.where(slots == slot_own[...], 1.0, 0.0).astype(bf16),
            jnp.where(slots == slot_in[...], 1.0, 0.0).astype(bf16),
        ],
        axis=1,
    )

    for i, far in ((0, ahead), (1, behind)):

        @pl.when(far > w)
        def _():
            pl.semaphore_wait(ready.at[i], 1)

    to_mate, to_ahead, to_behind = [], [], []

    def pass_on(q):
        to_mate[q].wait_recv()
        sums_out[q, AHEAD - 1] = (
            sums_out[q, AHEAD - 1].astype(f32) + mate_in[q, RELAY - 1].astype(f32)
        ).astype(bf16)
        copy = remote(sums_out.at[q, AHEAD - 1], ahead_in.at[q], ahead_sems, (q,), (ahead, n))
        copy.start()
        to_ahead.append(copy)

    for q in range(planes):
        for copy in cross[q]:
            copy.wait_recv()
        pair_values = jnp.concatenate([own_terms[q], cross_in[q]], axis=0)
        sums = jnp.dot(select, pair_values, preferred_element_type=f32)
        self_sum[q] = sums[:TB_DEV]
        for slot in (MATE, RELAY, AHEAD, BEHIND):
            sums_out[q, slot - 1] = sums[slot * TB_DEV : (slot + 1) * TB_DEV].astype(bf16)
        copy = remote(sums_out.at[q, pl.ds(0, 2)], mate_in.at[q], mate_sems, (q,), (mate, n))
        copy.start()
        to_mate.append(copy)
        copy = remote(
            sums_out.at[q, BEHIND - 1], behind_in.at[q], behind_sems, (q,), (behind, n)
        )
        copy.start()
        to_behind.append(copy)
        if q > 0:
            pass_on(q - 1)
    pass_on(planes - 1)

    for q in range(planes):
        to_behind[q].wait_recv()
        to_ahead[q].wait_recv()
        total = (
            self_sum[q]
            + mate_in[q, MATE - 1].astype(f32)
            + ahead_in[q].astype(f32)
            + behind_in[q].astype(f32)
        )
        if q < levels:
            covered = total > wet_limit * DENOM
            inverse[q] = jnp.where(covered, 1.0 / jnp.where(covered, total, 1.0), 0.0)
            continue
        k, level = divmod(q - levels, levels)
        staged[pl.ds(level, TB_DEV, stride=levels), :] = total * inverse[level]
        if level == levels - 1:
            for block in range(TB_DEV):
                out_ref[k, :, pl.ds(block * cells, cells)] = staged[
                    pl.ds(block * levels, levels), :
                ].astype(out_ref.dtype)
    for copies in cross:
        for copy in copies:
            copy.wait_send()
    for copy in to_mate + to_ahead + to_behind:
        copy.wait_send()


def by_kernel(src_field, src_depth, packed_counts, pair_source, pair_home, pair_count):
    wide_size = lax.axis_size("wide")
    fields, levels, _ = src_field.shape
    pairs, _, cells = packed_counts.shape
    tiles = src_depth.shape[0] // cells
    planes = (fields + 1) * levels
    sizes = (wide_size, fields, levels, tiles, cells, pairs)
    hbm = pl.BlockSpec(memory_space=pltpu.HBM)
    bf16, f32, i32 = jnp.bfloat16, jnp.float32, jnp.int32
    terms_shape = (planes, pairs, cells)
    block_shape = (TB_DEV, cells)
    copies = pltpu.SemaphoreType.DMA((2, planes))
    return pl.pallas_call(
        functools.partial(remap_kernel, sizes),
        out_shape=jax.ShapeDtypeStruct((fields, levels, TB_DEV * cells), bf16),
        in_specs=[hbm] * 6,
        out_specs=pl.BlockSpec(memory_space=pltpu.VMEM),
        scratch_shapes=[
            pltpu.VMEM(src_field.shape, bf16),
            pltpu.VMEM((tiles, cells), i32),
            pltpu.SMEM((pairs,), i32),
            pltpu.VMEM((1, pairs), i32),
            pltpu.SMEM((1,), i32),
            pltpu.VMEM((fields, levels, tiles * cells), bf16),
            pltpu.VMEM((1, pairs), i32),
            pltpu.VMEM((1, pairs), i32),
            pltpu.VMEM((pairs, cells // 2, cells), i32),
            pltpu.VMEM((pairs // 2, cells, 2 * cells), bf16),
            pltpu.VMEM((tiles, 2 * levels, cells), bf16),
            pltpu.VMEM((tiles, 2 * fields * levels, cells), bf16),
            pltpu.VMEM((2 * planes * (pairs + SKEW), cells), f32),
            pltpu.VMEM(terms_shape, bf16),
            pltpu.VMEM(terms_shape, bf16),
            pltpu.VMEM(terms_shape, bf16),
            pltpu.VMEM((planes,) + block_shape, f32),
            pltpu.VMEM((planes, 4) + block_shape, bf16),
            pltpu.VMEM((planes, 2) + block_shape, bf16),
            pltpu.VMEM((planes,) + block_shape, bf16),
            pltpu.VMEM((planes,) + block_shape, bf16),
            pltpu.VMEM((levels,) + block_shape, f32),
            pltpu.VMEM((TB_DEV * levels, cells), f32),
            pltpu.SemaphoreType.REGULAR((2,)),
            pltpu.SemaphoreType.DMA((LOADS,)),
            pltpu.SemaphoreType.DMA((5,)),
            pltpu.SemaphoreType.DMA((2, 2)),
            pltpu.SemaphoreType.DMA((2, LOADS)),
            pltpu.SemaphoreType.DMA((2, planes - EARLY)),
            copies,
            copies,
            copies,
        ],
        compiler_params=pltpu.CompilerParams(
            collective_id=0, has_side_effects=True, vmem_limit_bytes=VMEM_LIMIT
        ),
        name="remap",
    )(
        src_field,
        src_depth.reshape(tiles, cells),
        packed_counts,
        pair_source,
        pair_home.reshape(1, pairs),
        pair_count,
    )


def solution(mesh):
    placed = (
        P(None, "narrow", "wide"),
        P(("wide", "narrow")),
        P(("wide", "narrow"), None, None),
        P(("wide", "narrow")),
        P(("wide", "narrow")),
        P(("wide", "narrow")),
    )
    paired = mesh.shape["narrow"] == 2 and mesh.shape["wide"] % 2 == 0
    fits = paired and mesh.shape["wide"] > 2 * REACH and REACH == 2
    return jax.shard_map(
        by_kernel if fits else by_collectives,
        mesh=mesh,
        in_specs=placed,
        out_specs=P(None, "narrow", "wide"),
        check_vma=False,
    )
```

```python
import functools

import jax
import jax.numpy as jnp
from jax import lax
from jax.experimental import pallas as pl
from jax.experimental.pallas import tpu as pltpu
from jax.sharding import PartitionSpec as P

DENOM = 256
REACH = 2
TB_DEV = 64


wet_limit = 0.001


def passed_along(block, axis, distance):
    devices = range(lax.axis_size(axis))
    route = [((i - distance) % len(devices), i) for i in devices]
    return lax.ppermute(block, axis, route)


def unpack_counts(packed_words):
    return jnp.concatenate([packed_words % 65536, packed_words // 65536], axis=-2)


def block_sums(targets, received, block_count):
    owners = jnp.arange(block_count, dtype=jnp.int32)
    select = (targets[:, None] == owners[None, :]).astype(jnp.bfloat16)
    return jnp.einsum("rq,rlcb->lcqb", select, received, preferred_element_type=jnp.float32)


def by_collectives(src_field, src_depth, packed_counts, pair_source, pair_home, pair_count):
    narrow_size = lax.axis_size("narrow")
    wide_size = lax.axis_size("wide")
    field_vars = src_field.shape[0]
    components = field_vars + 1
    block_cells = packed_counts.shape[2]
    own_cells = src_depth.shape[0]
    own_tiles = own_cells // block_cells
    pair_slots = pair_source.shape[0]
    offset_count = 2 * REACH + 1
    capacity = max(2, 2 * pair_slots // offset_count)
    own_field = lax.all_to_all(src_field, "narrow", split_axis=2, concat_axis=1, tiled=True)
    levels = own_field.shape[1]
    part_levels = levels // narrow_size
    level_ids = jnp.arange(levels, dtype=jnp.int32)
    wet_levels = level_ids[:, None] < src_depth[None, :]
    masked = jnp.where(wet_levels[None, :, :], own_field, jnp.zeros_like(own_field))
    stacked = jnp.concatenate(
        [jnp.transpose(masked, (1, 0, 2)), wet_levels.astype(jnp.bfloat16)[:, None, :]], axis=1
    )
    by_tile = jnp.transpose(stacked.reshape(levels * components, own_tiles, block_cells), (1, 0, 2))
    picked = jnp.take(by_tile, pair_source, axis=0)
    weight = (unpack_counts(packed_counts).astype(jnp.float32) / DENOM).astype(jnp.bfloat16)
    pair_terms = lax.dot_general(
        picked, weight, (((2,), (2,)), ((0,), (0,))), preferred_element_type=jnp.float32
    )
    pair_terms = pair_terms.astype(jnp.bfloat16)
    is_live = jnp.arange(pair_slots, dtype=jnp.int32) < pair_count[0]
    wide_index = lax.axis_index("wide")
    destination = pair_home // TB_DEV
    local_block = pair_home % TB_DEV
    offset_index = (destination - wide_index + REACH + wide_size) % wide_size
    bound_for = (
        (offset_index[:, None] == jnp.arange(offset_count, dtype=jnp.int32)[None, :])
        & is_live[:, None]
    ).astype(jnp.int32)
    before = jnp.cumsum(bound_for, axis=0) - bound_for
    position = jnp.sum(before * bound_for, axis=1)
    slot_index = jnp.where(is_live, offset_index * capacity + position, offset_count * capacity)
    outgoing = (
        jnp.zeros((offset_count * capacity, levels * components, block_cells), jnp.bfloat16)
        .at[slot_index]
        .set(pair_terms, mode="drop")
    )
    targets = (
        jnp.full((offset_count * capacity,), TB_DEV, jnp.int32)
        .at[slot_index]
        .set(local_block, mode="drop")
    )
    outgoing = outgoing.reshape(offset_count, capacity, levels, components, block_cells)
    targets = targets.reshape(offset_count, capacity)
    shift_list = [shift_by for shift_by in range(-REACH, REACH + 1) if shift_by != 0]
    partial_value = block_sums(targets[REACH], outgoing[REACH], TB_DEV)
    for shift_by in shift_list:
        moved_terms, moved_owners = passed_along(
            (outgoing[REACH + shift_by], targets[REACH + shift_by]), "wide", shift_by
        )
        partial_value = partial_value + block_sums(moved_owners, moved_terms, TB_DEV)
    block_totals = lax.psum_scatter(partial_value, "narrow", scatter_dimension=0, tiled=True)
    numerators = block_totals[:, :field_vars]
    wet_total = block_totals[:, field_vars]
    covered = wet_total > wet_limit
    safe_wet = jnp.where(covered, wet_total, jnp.ones_like(wet_total))
    result = jnp.where(covered[:, None], numerators / safe_wet[:, None], jnp.zeros_like(numerators))
    result = jnp.transpose(result, (1, 0, 2, 3)).reshape(
        field_vars, part_levels, TB_DEV * block_cells
    )
    return result.astype(jnp.bfloat16)


SELF, MATE, RELAY, AHEAD, BEHIND = range(5)
LOADS = 4
EARLY = 4
SKEW = 8
LAG = 3
LATE = 2
VMEM_LIMIT = 26 * 2**20


def remap_kernel(
    sizes,
    field_hbm,
    depth_hbm,
    packed_hbm,
    source_hbm,
    home_hbm,
    count,
    out_ref,
    field,
    depth,
    source,
    home,
    field_in,
    slot_own,
    slot_in,
    words,
    weight,
    wets,
    fields_at,
    terms,
    cross_out,
    cross_in,
    own_terms,
    self_sum,
    sums_out,
    mate_in,
    ahead_in,
    behind_in,
    inverse,
    staged,
    ready,
    load_sems,
    small_sems,
    entry_sems,
    early_sems,
    cross_sems,
    mate_sems,
    ahead_sems,
    behind_sems,
):
    wide_size, fields, levels, tiles, cells, pairs = sizes
    planes = (fields + 1) * levels
    pitch = pairs + SKEW
    f32, bf16, i32 = jnp.float32, jnp.bfloat16, jnp.int32
    w = lax.axis_index("wide")
    n = lax.axis_index("narrow")
    other = 1 - n
    sign = 1 - 2 * lax.rem(w, 2)
    mate = w + sign
    ahead = lax.rem(w + 2 * sign + wide_size, wide_size)
    behind = lax.rem(w - 2 * sign + wide_size, wide_size)

    def signal(sem, place):
        pl.semaphore_signal(sem, inc=1, device_id=place, device_id_type=pl.DeviceIdType.MESH)

    barrier = pltpu.get_barrier_semaphore()
    signal(barrier, (w, other))
    signal(barrier, (mate, n))
    for far in (ahead, behind):

        @pl.when(far > w)
        def _():
            signal(barrier, (far, n))

    small = []
    for i, (src, dst) in enumerate(
        (
            (field_hbm, field),
            (home_hbm, home),
            (depth_hbm, depth),
            (source_hbm, source),
        )
    ):
        load = pltpu.make_async_copy(src, dst, small_sems.at[i])
        load.start()
        small.append(load)
    per_load = pairs // LOADS
    loads = []
    for i in range(LOADS):
        span = pl.ds(i * per_load, per_load)
        load = pltpu.make_async_copy(packed_hbm.at[span], words.at[span], load_sems.at[i])
        load.start()
        loads.append(load)

    def remote(src, dst, sems, index, place):
        return pltpu.make_async_remote_copy(
            src_ref=src,
            dst_ref=dst,
            send_sem=sems.at[(0,) + index],
            recv_sem=sems.at[(1,) + index],
            device_id=place,
            device_id_type=pl.DeviceIdType.MESH,
        )

    small[1].wait()
    wide_home = lax.div(home[...], TB_DEV)
    offset = lax.rem(wide_home - w + REACH + wide_size, wide_size) - REACH
    toward = offset * sign
    slot = jnp.where(toward > 0, 2 * toward - 1, -2 * toward)
    is_live = lax.broadcasted_iota(i32, (1, pairs), 1) < count[0]
    slot_own[...] = jnp.where(is_live, slot * TB_DEV + home[...] - wide_home * TB_DEV, -1)
    own_cells = tiles * cells
    theirs = pl.ds(pl.multiple_of(other * own_cells, own_cells), own_cells)
    pl.semaphore_wait(barrier, 2 + (ahead < w).astype(i32) + (behind < w).astype(i32))
    for i, far in ((1, ahead), (0, behind)):

        @pl.when(far < w)
        def _():
            signal(ready.at[i], (far, n))

    small[0].wait()
    entry = [remote(field.at[:, :, theirs], field_in, entry_sems, (0,), (w, other))]
    entry[0].start()
    entry.append(remote(slot_own, slot_in, entry_sems, (1,), (w, other)))
    entry[1].start()

    small[2].wait()
    rows = lax.broadcasted_iota(i32, (2 * levels, cells), 0)
    level_of = jnp.where(rows < levels, rows + other * levels, rows - levels + n * levels)
    for tile in range(tiles):
        wet = level_of < depth[pl.ds(tile, 1), :]
        wets[tile] = jnp.where(wet, 1.0, 0.0).astype(bf16)

    half = cells // 2

    def unpack(first):
        for u in range(per_load):
            p = first + u
            word = words[p]
            lanes = pl.ds((u % 2) * cells, cells)
            low = (word & 65535).astype(f32).astype(bf16)
            high = (word >> 16).astype(f32).astype(bf16)
            weight[(first + u) // 2, pl.ds(0, half), lanes] = low
            weight[(first + u) // 2, pl.ds(half, half), lanes] = high

    def multiply(values_of, count, base, first):
        zero = jnp.zeros((count, cells), bf16)
        for u in range(0, per_load, 2):
            p = first + u
            left = jnp.concatenate([values_of[source[p]], zero], axis=1)
            right = jnp.concatenate([zero, values_of[source[p + 1]]], axis=1)
            term = lax.dot_general(
                jnp.concatenate([left, right], axis=0),
                weight[p // 2],
                (((1,), (1,)), ((), ())),
                preferred_element_type=f32,
            )
            terms[pl.ds(base * pitch + p, count, stride=pitch), :] = term[:count]
            terms[pl.ds(base * pitch + p + 1, count, stride=pitch), :] = term[count:]

    def rounded(row, start, count):
        return terms[pl.ds(row * pitch + start, count), :].astype(bf16)

    small[3].wait()
    loads[0].wait()
    unpack(0)
    cross = [[] for _ in range(planes)]
    for batch in range(LOADS):
        first = batch * per_load
        if batch + 1 < LOADS:
            loads[batch + 1].wait()
            unpack(first + per_load)
        multiply(wets, 2 * levels, 0, first)
        span = pl.ds(first, per_load)
        for q in range(EARLY):
            cross_out[q, span, :] = rounded(q, first, per_load)
        some = pl.ds(0, EARLY)
        copy = remote(
            cross_out.at[some, span, :], cross_in.at[some, span, :],
            early_sems, (batch,), (w, other),
        )
        copy.start()
        cross[0].append(copy)

    def send_terms(q):
        cross_out[q] = rounded(q if q < levels else q + levels, 0, pairs)
        copy = remote(cross_out.at[q], cross_in.at[q], cross_sems, (q - EARLY,), (w, other))
        copy.start()
        cross[q].append(copy)

    for q in range(EARLY, levels):
        send_terms(q)

    level_ids = lax.broadcasted_iota(i32, (levels, cells), 0)

    def stack(side, group, read):
        for tile in range(tiles):
            wet = level_ids + group * levels < depth[pl.ds(tile, 1), :]
            values = [jnp.where(wet, read(k, tile).astype(f32), 0.0) for k in range(fields)]
            fields_at[tile, pl.ds(side * fields * levels, fields * levels), :] = (
                jnp.concatenate(values, axis=0).astype(bf16)
            )

    own_start = n * own_cells
    stack(
        1,
        n,
        lambda k, tile: field[k, :, pl.ds(pl.multiple_of(own_start + tile * cells, cells), cells)],
    )
    for q in range(levels):
        own_terms[q] = rounded(q + levels, 0, pairs)

    entry[0].wait()
    stack(0, other, lambda k, tile: field_in[k, :, pl.ds(tile * cells, cells)])

    def batch_of_fields(batch, carry):
        multiply(fields_at, 2 * fields * levels, 2 * levels, batch * per_load)
        return carry

    lax.fori_loop(0, LOADS, batch_of_fields, 0)
    for q in range(levels, planes):
        send_terms(q)
    for q in range(levels, planes):
        own_terms[q] = rounded(q + levels + fields * levels, 0, pairs)

    entry[1].wait()
    slots = lax.broadcasted_iota(i32, (5 * TB_DEV, pairs), 0)
    select = jnp.concatenate(
        [
            jnp.where(slots == slot_own[...], 1.0, 0.0).astype(bf16),
            jnp.where(slots == slot_in[...], 1.0, 0.0).astype(bf16),
        ],
        axis=1,
    )

    for i, far in ((0, ahead), (1, behind)):

        @pl.when(far > w)
        def _():
            pl.semaphore_wait(ready.at[i], 1)

    to_mate, to_ahead, to_behind = [], [], []

    def pass_on(q):
        to_mate[q].wait_recv()
        sums_out[q, AHEAD - 1] = (
            sums_out[q, AHEAD - 1].astype(f32) + mate_in[q, RELAY - 1].astype(f32)
        ).astype(bf16)
        copy = remote(sums_out.at[q, AHEAD - 1], ahead_in.at[q], ahead_sems, (q,), (ahead, n))
        copy.start()
        to_ahead.append(copy)

    for q in range(planes):
        for copy in cross[q]:
            copy.wait_recv()
        pair_values = jnp.concatenate([own_terms[q], cross_in[q]], axis=0)
        sums = jnp.dot(select, pair_values, preferred_element_type=f32)
        self_sum[q] = sums[:TB_DEV]
        for slot in (MATE, RELAY, AHEAD, BEHIND):
            sums_out[q, slot - 1] = sums[slot * TB_DEV : (slot + 1) * TB_DEV].astype(bf16)
        copy = remote(sums_out.at[q, pl.ds(0, 2)], mate_in.at[q], mate_sems, (q,), (mate, n))
        copy.start()
        to_mate.append(copy)
        copy = remote(
            sums_out.at[q, BEHIND - 1], behind_in.at[q], behind_sems, (q,), (behind, n)
        )
        copy.start()
        to_behind.append(copy)
        if q >= LAG:
            pass_on(q - LAG)
    for q in range(planes - LAG, planes):
        pass_on(q)

    for q in range(planes):
        if q == planes - 1:
            for copies in cross:
                for copy in copies:
                    copy.wait_send()
            for copies in (to_mate, to_behind, to_ahead):
                for copy in copies[: planes - LATE]:
                    copy.wait_send()
        to_behind[q].wait_recv()
        to_ahead[q].wait_recv()
        total = (
            self_sum[q]
            + mate_in[q, MATE - 1].astype(f32)
            + ahead_in[q].astype(f32)
            + behind_in[q].astype(f32)
        )
        if q < levels:
            covered = total > wet_limit * DENOM
            inverse[q] = jnp.where(covered, 1.0 / jnp.where(covered, total, 1.0), 0.0)
            continue
        k, level = divmod(q - levels, levels)
        staged[pl.ds(level, TB_DEV, stride=levels), :] = total * inverse[level]
        if level == levels - 1:
            for block in range(TB_DEV):
                out_ref[k, :, pl.ds(block * cells, cells)] = staged[
                    pl.ds(block * levels, levels), :
                ].astype(out_ref.dtype)
    for copies in (to_mate, to_behind, to_ahead):
        for copy in copies[planes - LATE :]:
            copy.wait_send()


def by_kernel(src_field, src_depth, packed_counts, pair_source, pair_home, pair_count):
    wide_size = lax.axis_size("wide")
    fields, levels, _ = src_field.shape
    pairs, _, cells = packed_counts.shape
    tiles = src_depth.shape[0] // cells
    planes = (fields + 1) * levels
    sizes = (wide_size, fields, levels, tiles, cells, pairs)
    hbm = pl.BlockSpec(memory_space=pltpu.HBM)
    bf16, f32, i32 = jnp.bfloat16, jnp.float32, jnp.int32
    terms_shape = (planes, pairs, cells)
    block_shape = (TB_DEV, cells)
    copies = pltpu.SemaphoreType.DMA((2, planes))
    operands = (
        src_field,
        src_depth.reshape(tiles, cells),
        packed_counts,
        pair_source,
        pair_home.reshape(1, pairs),
    )
    return pl.pallas_call(
        functools.partial(remap_kernel, sizes),
        out_shape=jax.ShapeDtypeStruct((fields, levels, TB_DEV * cells), bf16),
        in_specs=[hbm] * len(operands) + [pl.BlockSpec(memory_space=pltpu.SMEM)],
        out_specs=pl.BlockSpec(memory_space=pltpu.VMEM),
        scratch_shapes=[
            pltpu.VMEM(src_field.shape, bf16),
            pltpu.VMEM((tiles, cells), i32),
            pltpu.SMEM((pairs,), i32),
            pltpu.VMEM((1, pairs), i32),
            pltpu.VMEM((fields, levels, tiles * cells), bf16),
            pltpu.VMEM((1, pairs), i32),
            pltpu.VMEM((1, pairs), i32),
            pltpu.VMEM((pairs, cells // 2, cells), i32),
            pltpu.VMEM((pairs // 2, cells, 2 * cells), bf16),
            pltpu.VMEM((tiles, 2 * levels, cells), bf16),
            pltpu.VMEM((tiles, 2 * fields * levels, cells), bf16),
            pltpu.VMEM((2 * planes * (pairs + SKEW), cells), f32),
            pltpu.VMEM(terms_shape, bf16),
            pltpu.VMEM(terms_shape, bf16),
            pltpu.VMEM(terms_shape, bf16),
            pltpu.VMEM((planes,) + block_shape, f32),
            pltpu.VMEM((planes, 4) + block_shape, bf16),
            pltpu.VMEM((planes, 2) + block_shape, bf16),
            pltpu.VMEM((planes,) + block_shape, bf16),
            pltpu.VMEM((planes,) + block_shape, bf16),
            pltpu.VMEM((levels,) + block_shape, f32),
            pltpu.VMEM((TB_DEV * levels, cells), f32),
            pltpu.SemaphoreType.REGULAR((2,)),
            pltpu.SemaphoreType.DMA((LOADS,)),
            pltpu.SemaphoreType.DMA((4,)),
            pltpu.SemaphoreType.DMA((2, 2)),
            pltpu.SemaphoreType.DMA((2, LOADS)),
            pltpu.SemaphoreType.DMA((2, planes - EARLY)),
            copies,
            copies,
            copies,
        ],
        compiler_params=pltpu.CompilerParams(
            collective_id=0, has_side_effects=True, vmem_limit_bytes=VMEM_LIMIT
        ),
        name="remap",
    )(
        *(pltpu.with_memory_space_constraint(x, pltpu.HBM) for x in operands),
        pair_count,
    )


def solution(mesh):
    placed = (
        P(None, "narrow", "wide"),
        P(("wide", "narrow")),
        P(("wide", "narrow"), None, None),
        P(("wide", "narrow")),
        P(("wide", "narrow")),
        P(("wide", "narrow")),
    )
    paired = mesh.shape["narrow"] == 2 and mesh.shape["wide"] % 2 == 0
    fits = paired and mesh.shape["wide"] > 2 * REACH and REACH == 2
    return jax.shard_map(
        by_kernel if fits else by_collectives,
        mesh=mesh,
        in_specs=placed,
        out_specs=P(None, "narrow", "wide"),
        check_vma=False,
    )
```

```python
import functools

import jax
import jax.numpy as jnp
from jax import lax
from jax.experimental import pallas as pl
from jax.experimental.pallas import tpu as pltpu
from jax.sharding import PartitionSpec as P

DENOM = 256
REACH = 2
TB_DEV = 64


wet_limit = 0.001


def passed_along(block, axis, distance):
    devices = range(lax.axis_size(axis))
    route = [((i - distance) % len(devices), i) for i in devices]
    return lax.ppermute(block, axis, route)


def unpack_counts(packed_words):
    return jnp.concatenate([packed_words % 65536, packed_words // 65536], axis=-2)


def block_sums(targets, received, block_count):
    owners = jnp.arange(block_count, dtype=jnp.int32)
    select = (targets[:, None] == owners[None, :]).astype(jnp.bfloat16)
    return jnp.einsum("rq,rlcb->lcqb", select, received, preferred_element_type=jnp.float32)


def by_collectives(src_field, src_depth, packed_counts, pair_source, pair_home, pair_count):
    narrow_size = lax.axis_size("narrow")
    wide_size = lax.axis_size("wide")
    field_vars = src_field.shape[0]
    components = field_vars + 1
    block_cells = packed_counts.shape[2]
    own_cells = src_depth.shape[0]
    own_tiles = own_cells // block_cells
    pair_slots = pair_source.shape[0]
    offset_count = 2 * REACH + 1
    capacity = max(2, 2 * pair_slots // offset_count)
    own_field = lax.all_to_all(src_field, "narrow", split_axis=2, concat_axis=1, tiled=True)
    levels = own_field.shape[1]
    part_levels = levels // narrow_size
    level_ids = jnp.arange(levels, dtype=jnp.int32)
    wet_levels = level_ids[:, None] < src_depth[None, :]
    masked = jnp.where(wet_levels[None, :, :], own_field, jnp.zeros_like(own_field))
    stacked = jnp.concatenate(
        [jnp.transpose(masked, (1, 0, 2)), wet_levels.astype(jnp.bfloat16)[:, None, :]], axis=1
    )
    by_tile = jnp.transpose(stacked.reshape(levels * components, own_tiles, block_cells), (1, 0, 2))
    picked = jnp.take(by_tile, pair_source, axis=0)
    weight = (unpack_counts(packed_counts).astype(jnp.float32) / DENOM).astype(jnp.bfloat16)
    pair_terms = lax.dot_general(
        picked, weight, (((2,), (2,)), ((0,), (0,))), preferred_element_type=jnp.float32
    )
    pair_terms = pair_terms.astype(jnp.bfloat16)
    is_live = jnp.arange(pair_slots, dtype=jnp.int32) < pair_count[0]
    wide_index = lax.axis_index("wide")
    destination = pair_home // TB_DEV
    local_block = pair_home % TB_DEV
    offset_index = (destination - wide_index + REACH + wide_size) % wide_size
    bound_for = (
        (offset_index[:, None] == jnp.arange(offset_count, dtype=jnp.int32)[None, :])
        & is_live[:, None]
    ).astype(jnp.int32)
    before = jnp.cumsum(bound_for, axis=0) - bound_for
    position = jnp.sum(before * bound_for, axis=1)
    slot_index = jnp.where(is_live, offset_index * capacity + position, offset_count * capacity)
    outgoing = (
        jnp.zeros((offset_count * capacity, levels * components, block_cells), jnp.bfloat16)
        .at[slot_index]
        .set(pair_terms, mode="drop")
    )
    targets = (
        jnp.full((offset_count * capacity,), TB_DEV, jnp.int32)
        .at[slot_index]
        .set(local_block, mode="drop")
    )
    outgoing = outgoing.reshape(offset_count, capacity, levels, components, block_cells)
    targets = targets.reshape(offset_count, capacity)
    shift_list = [shift_by for shift_by in range(-REACH, REACH + 1) if shift_by != 0]
    partial_value = block_sums(targets[REACH], outgoing[REACH], TB_DEV)
    for shift_by in shift_list:
        moved_terms, moved_owners = passed_along(
            (outgoing[REACH + shift_by], targets[REACH + shift_by]), "wide", shift_by
        )
        partial_value = partial_value + block_sums(moved_owners, moved_terms, TB_DEV)
    block_totals = lax.psum_scatter(partial_value, "narrow", scatter_dimension=0, tiled=True)
    numerators = block_totals[:, :field_vars]
    wet_total = block_totals[:, field_vars]
    covered = wet_total > wet_limit
    safe_wet = jnp.where(covered, wet_total, jnp.ones_like(wet_total))
    result = jnp.where(covered[:, None], numerators / safe_wet[:, None], jnp.zeros_like(numerators))
    result = jnp.transpose(result, (1, 0, 2, 3)).reshape(
        field_vars, part_levels, TB_DEV * block_cells
    )
    return result.astype(jnp.bfloat16)


SELF, MATE, RELAY, AHEAD, BEHIND = range(5)
LOADS = 4
EARLY = 2
SKEW = 8
LAG = 2
BETWEEN = 3
LAST_GROUPS = (4, 1, 1, 1, 1)
VMEM_LIMIT = 26 * 2**20


def remap_kernel(
    sizes,
    field_hbm,
    depth_hbm,
    packed_hbm,
    source_hbm,
    home_hbm,
    count,
    out_ref,
    field,
    depth,
    source,
    home,
    field_in,
    slot_own,
    slot_in,
    words,
    weight,
    wets,
    fields_at,
    terms,
    select,
    cross_out,
    cross_in,
    own_terms,
    self_sum,
    sums_out,
    mate_in,
    far_in,
    inverse,
    staged,
    ready,
    load_sems,
    small_sems,
    entry_sems,
    sent_sems,
    cross_sems,
    mate_sems,
    far_sems,
):
    wide_size, fields, levels, tiles, cells, pairs = sizes
    planes = (fields + 1) * levels
    pitch = pairs + SKEW
    f32, bf16, i32 = jnp.float32, jnp.bfloat16, jnp.int32
    w = lax.axis_index("wide")
    n = lax.axis_index("narrow")
    other = 1 - n
    sign = 1 - 2 * lax.rem(w, 2)
    mate = w + sign
    ahead = lax.rem(w + 2 * sign + wide_size, wide_size)
    behind = lax.rem(w - 2 * sign + wide_size, wide_size)

    def signal(sem, place):
        pl.semaphore_signal(sem, inc=1, device_id=place, device_id_type=pl.DeviceIdType.MESH)

    barrier = pltpu.get_barrier_semaphore()
    signal(barrier, (w, other))
    signal(barrier, (mate, n))
    for far in (ahead, behind):

        @pl.when(far > w)
        def _():
            signal(barrier, (far, n))

    small = []
    for i, (src, dst) in enumerate(
        (
            (field_hbm, field),
            (home_hbm, home),
            (depth_hbm, depth),
            (source_hbm, source),
        )
    ):
        load = pltpu.make_async_copy(src, dst, small_sems.at[i])
        load.start()
        small.append(load)
    per_load = pairs // LOADS
    loads = []
    for i in range(LOADS):
        span = pl.ds(i * per_load, per_load)
        load = pltpu.make_async_copy(packed_hbm.at[span], words.at[span], load_sems.at[i])
        load.start()
        loads.append(load)

    def remote(src, dst, sent, received, place):
        return pltpu.make_async_remote_copy(
            src_ref=src,
            dst_ref=dst,
            send_sem=sent,
            recv_sem=received,
            device_id=place,
            device_id_type=pl.DeviceIdType.MESH,
        )

    small[1].wait()
    wide_home = lax.div(home[...], TB_DEV)
    offset = lax.rem(wide_home - w + REACH + wide_size, wide_size) - REACH
    toward = offset * sign
    slot = jnp.where(toward > 0, 2 * toward - 1, -2 * toward)
    is_live = lax.broadcasted_iota(i32, (1, pairs), 1) < count[0]
    slot_own[...] = jnp.where(is_live, slot * TB_DEV + home[...] - wide_home * TB_DEV, -1)
    own_cells = tiles * cells
    theirs = pl.ds(pl.multiple_of(other * own_cells, own_cells), own_cells)
    pl.semaphore_wait(barrier, 2 + (ahead < w).astype(i32) + (behind < w).astype(i32))
    for i, far in ((1, ahead), (0, behind)):

        @pl.when(far < w)
        def _():
            signal(ready.at[i], (far, n))

    small[0].wait()
    entry = [
        remote(field.at[:, :, theirs], field_in, entry_sems.at[0], entry_sems.at[1], (w, other))
    ]
    entry[0].start()
    entry.append(remote(slot_own, slot_in, entry_sems.at[2], entry_sems.at[3], (w, other)))
    entry[1].start()

    small[2].wait()
    rows = lax.broadcasted_iota(i32, (2 * levels, cells), 0)
    level_of = jnp.where(rows < levels, rows + other * levels, rows - levels + n * levels)
    for tile in range(tiles):
        wet = level_of < depth[pl.ds(tile, 1), :]
        wets[tile] = jnp.where(wet, 1.0, 0.0).astype(bf16)

    half = cells // 2

    def unpack(first):
        for u in range(per_load):
            p = first + u
            word = words[p]
            lanes = pl.ds((u % 2) * cells, cells)
            low = (word & 65535).astype(f32).astype(bf16)
            high = (word >> 16).astype(f32).astype(bf16)
            weight[(first + u) // 2, pl.ds(0, half), lanes] = low
            weight[(first + u) // 2, pl.ds(half, half), lanes] = high

    def multiply(values_of, count, base, first):
        zero = jnp.zeros((count, cells), bf16)
        for u in range(0, per_load, 2):
            p = first + u
            left = jnp.concatenate([values_of[source[p]], zero], axis=1)
            right = jnp.concatenate([zero, values_of[source[p + 1]]], axis=1)
            term = lax.dot_general(
                jnp.concatenate([left, right], axis=0),
                weight[p // 2],
                (((1,), (1,)), ((), ())),
                preferred_element_type=f32,
            )
            terms[pl.ds(base * pitch + p, count, stride=pitch), :] = term[:count]
            terms[pl.ds(base * pitch + p + 1, count, stride=pitch), :] = term[count:]

    def rounded(row, start, count):
        return terms[pl.ds(row * pitch + start, count), :].astype(bf16)

    small[3].wait()
    loads[0].wait()
    unpack(0)
    sent_cross, sent_mate, sent_ahead, sent_behind = (sent_sems.at[i] for i in range(4))
    some = pl.ds(0, EARLY)
    for batch in range(LOADS):
        first = batch * per_load
        if batch + 1 < LOADS:
            loads[batch + 1].wait()
            unpack(first + per_load)
        multiply(wets, 2 * levels, 0, first)
        span = pl.ds(first, per_load)
        for q in range(EARLY):
            cross_out[q, span, :] = rounded(q, first, per_load)
        remote(
            cross_out.at[some, span, :], cross_in.at[some, span, :],
            sent_cross, cross_sems.at[0], (w, other),
        ).start()

    def cross(some, i):
        return remote(
            cross_out.at[some], cross_in.at[some], sent_cross, cross_sems.at[i], (w, other)
        )

    def send_terms(q):
        cross_out[q] = rounded(q if q < levels else q + levels, 0, pairs)
        cross(pl.ds(q, 1), q - EARLY + 1).start()

    for q in range(EARLY, levels):
        send_terms(q)

    level_ids = lax.broadcasted_iota(i32, (levels, cells), 0)

    def stack(side, group, read):
        for tile in range(tiles):
            wet = level_ids + group * levels < depth[pl.ds(tile, 1), :]
            values = [jnp.where(wet, read(k, tile).astype(f32), 0.0) for k in range(fields)]
            fields_at[tile, pl.ds(side * fields * levels, fields * levels), :] = (
                jnp.concatenate(values, axis=0).astype(bf16)
            )

    own_start = n * own_cells
    stack(
        1,
        n,
        lambda k, tile: field[k, :, pl.ds(pl.multiple_of(own_start + tile * cells, cells), cells)],
    )
    for q in range(levels):
        own_terms[q] = rounded(q + levels, 0, pairs)

    entry[1].wait()
    slots = lax.broadcasted_iota(i32, (5 * TB_DEV, pairs), 0)
    select[:, pl.ds(0, pairs)] = jnp.where(slots == slot_own[...], 1.0, 0.0).astype(bf16)
    select[:, pl.ds(pairs, pairs)] = jnp.where(slots == slot_in[...], 1.0, 0.0).astype(bf16)

    for i, far in ((0, ahead), (1, behind)):

        @pl.when(far > w)
        def _():
            pl.semaphore_wait(ready.at[i], 1)

    groups = (planes - sum(LAST_GROUPS),) + LAST_GROUPS
    group_of = [g for g, size in enumerate(groups) for _ in range(size)]

    def to_mate(some, i):
        place = (mate, n)
        src, dst = sums_out.at[some, pl.ds(0, 2)], mate_in.at[some]
        return remote(src, dst, sent_mate, mate_sems.at[i], place)

    def to_ahead(some, i):
        src, dst = sums_out.at[some, pl.ds(AHEAD - 1, 1)], far_in.at[some, pl.ds(0, 1)]
        return remote(src, dst, sent_ahead, far_sems.at[i], (ahead, n))

    def to_behind(some, i):
        src, dst = sums_out.at[some, pl.ds(BEHIND - 1, 1)], far_in.at[some, pl.ds(1, 1)]
        return remote(src, dst, sent_behind, far_sems.at[i], (behind, n))

    def pass_on(q):
        to_mate(pl.ds(q, 1), q).wait_recv()
        sums_out[q, AHEAD - 1] = (
            sums_out[q, AHEAD - 1].astype(f32) + mate_in[q, RELAY - 1].astype(f32)
        ).astype(bf16)
        to_ahead(pl.ds(q, 1), group_of[q]).start()

    def add_up(q):
        if q == 0:
            cross(some, 0).wait_recv()
        if q >= EARLY:
            cross(pl.ds(q, 1), q - EARLY + 1).wait_recv()
        pair_values = jnp.concatenate([own_terms[q], cross_in[q]], axis=0)
        sums = jnp.dot(select[...], pair_values, preferred_element_type=f32)
        self_sum[q] = sums[:TB_DEV]
        for slot in (MATE, RELAY, AHEAD, BEHIND):
            sums_out[q, slot - 1] = sums[slot * TB_DEV : (slot + 1) * TB_DEV].astype(bf16)
        to_mate(pl.ds(q, 1), q).start()
        to_behind(pl.ds(q, 1), group_of[q]).start()
        if q >= LAG:
            pass_on(q - LAG)

    entry[0].wait()
    stack(0, other, lambda k, tile: field_in[k, :, pl.ds(tile * cells, cells)])
    for batch in range(LOADS):
        multiply(fields_at, 2 * fields * levels, 2 * levels, batch * per_load)
        if batch < BETWEEN:
            add_up(batch)
    for q in range(levels, planes):
        send_terms(q)
    for q in range(levels, planes):
        own_terms[q] = rounded(q + levels + fields * levels, 0, pairs)
    for q in range(BETWEEN, planes):
        add_up(q)
    for q in range(planes - LAG, planes):
        pass_on(q)

    for q in range(planes):
        if q == groups[0]:
            cross(pl.ds(0, planes), 0).wait_send()
        if q == 0 or group_of[q] != group_of[q - 1]:
            arrived = far_in.at[pl.ds(q, groups[group_of[q]])]
            remote(arrived, arrived, sent_ahead, far_sems.at[group_of[q]], (ahead, n)).wait_recv()
        total = (
            self_sum[q]
            + mate_in[q, MATE - 1].astype(f32)
            + far_in[q, 0].astype(f32)
            + far_in[q, 1].astype(f32)
        )
        if q < levels:
            covered = total > wet_limit * DENOM
            inverse[q] = jnp.where(covered, 1.0 / jnp.where(covered, total, 1.0), 0.0)
            continue
        k, level = divmod(q - levels, levels)
        staged[pl.ds(level, TB_DEV, stride=levels), :] = total * inverse[level]
        if level == levels - 1:
            for block in range(TB_DEV):
                out_ref[k, :, pl.ds(block * cells, cells)] = staged[
                    pl.ds(block * levels, levels), :
                ].astype(out_ref.dtype)
    for copy in (to_mate, to_behind, to_ahead):
        copy(pl.ds(0, planes), 0).wait_send()


def by_kernel(src_field, src_depth, packed_counts, pair_source, pair_home, pair_count):
    wide_size = lax.axis_size("wide")
    fields, levels, _ = src_field.shape
    pairs, _, cells = packed_counts.shape
    tiles = src_depth.shape[0] // cells
    planes = (fields + 1) * levels
    sizes = (wide_size, fields, levels, tiles, cells, pairs)
    hbm = pl.BlockSpec(memory_space=pltpu.HBM)
    bf16, f32, i32 = jnp.bfloat16, jnp.float32, jnp.int32
    terms_shape = (planes, pairs, cells)
    block_shape = (TB_DEV, cells)
    operands = (
        src_field,
        src_depth.reshape(tiles, cells),
        packed_counts,
        pair_source,
        pair_home.reshape(1, pairs),
    )
    return pl.pallas_call(
        functools.partial(remap_kernel, sizes),
        out_shape=jax.ShapeDtypeStruct((fields, levels, TB_DEV * cells), bf16),
        in_specs=[hbm] * len(operands) + [pl.BlockSpec(memory_space=pltpu.SMEM)],
        out_specs=pl.BlockSpec(memory_space=pltpu.VMEM),
        scratch_shapes=[
            pltpu.VMEM(src_field.shape, bf16),
            pltpu.VMEM((tiles, cells), i32),
            pltpu.SMEM((pairs,), i32),
            pltpu.VMEM((1, pairs), i32),
            pltpu.VMEM((fields, levels, tiles * cells), bf16),
            pltpu.VMEM((1, pairs), i32),
            pltpu.VMEM((1, pairs), i32),
            pltpu.VMEM((pairs, cells // 2, cells), i32),
            pltpu.VMEM((pairs // 2, cells, 2 * cells), bf16),
            pltpu.VMEM((tiles, 2 * levels, cells), bf16),
            pltpu.VMEM((tiles, 2 * fields * levels, cells), bf16),
            pltpu.VMEM((2 * planes * (pairs + SKEW), cells), f32),
            pltpu.VMEM((5 * TB_DEV, 2 * pairs), bf16),
            pltpu.VMEM(terms_shape, bf16),
            pltpu.VMEM(terms_shape, bf16),
            pltpu.VMEM(terms_shape, bf16),
            pltpu.VMEM((planes,) + block_shape, f32),
            pltpu.VMEM((planes, 4) + block_shape, bf16),
            pltpu.VMEM((planes, 2) + block_shape, bf16),
            pltpu.VMEM((planes, 2) + block_shape, bf16),
            pltpu.VMEM((levels,) + block_shape, f32),
            pltpu.VMEM((TB_DEV * levels, cells), f32),
            pltpu.SemaphoreType.REGULAR((2,)),
            pltpu.SemaphoreType.DMA((LOADS,)),
            pltpu.SemaphoreType.DMA((4,)),
            pltpu.SemaphoreType.DMA((4,)),
            pltpu.SemaphoreType.DMA((4,)),
            pltpu.SemaphoreType.DMA((planes - EARLY + 1,)),
            pltpu.SemaphoreType.DMA((planes,)),
            pltpu.SemaphoreType.DMA((1 + len(LAST_GROUPS),)),
        ],
        compiler_params=pltpu.CompilerParams(
            collective_id=0, has_side_effects=True, vmem_limit_bytes=VMEM_LIMIT
        ),
        name="remap",
    )(
        *(pltpu.with_memory_space_constraint(x, pltpu.HBM) for x in operands),
        pair_count,
    )


def solution(mesh):
    placed = (
        P(None, "narrow", "wide"),
        P(("wide", "narrow")),
        P(("wide", "narrow"), None, None),
        P(("wide", "narrow")),
        P(("wide", "narrow")),
        P(("wide", "narrow")),
    )
    paired = mesh.shape["narrow"] == 2 and mesh.shape["wide"] % 2 == 0
    fits = paired and mesh.shape["wide"] > 2 * REACH and REACH == 2
    return jax.shard_map(
        by_kernel if fits else by_collectives,
        mesh=mesh,
        in_specs=placed,
        out_specs=P(None, "narrow", "wide"),
        check_vma=False,
    )
```

```python
import functools

import jax
import jax.numpy as jnp
from jax import lax
from jax.experimental import pallas as pl
from jax.experimental.pallas import tpu as pltpu
from jax.sharding import PartitionSpec as P

DENOM = 256
REACH = 2
TB_DEV = 64


wet_limit = 0.001


def passed_along(block, axis, distance):
    devices = range(lax.axis_size(axis))
    route = [((i - distance) % len(devices), i) for i in devices]
    return lax.ppermute(block, axis, route)


def unpack_counts(packed_words):
    return jnp.concatenate([packed_words % 65536, packed_words // 65536], axis=-2)


def block_sums(targets, received, block_count):
    owners = jnp.arange(block_count, dtype=jnp.int32)
    select = (targets[:, None] == owners[None, :]).astype(jnp.bfloat16)
    return jnp.einsum("rq,rlcb->lcqb", select, received, preferred_element_type=jnp.float32)


def by_collectives(src_field, src_depth, packed_counts, pair_source, pair_home, pair_count):
    narrow_size = lax.axis_size("narrow")
    wide_size = lax.axis_size("wide")
    field_vars = src_field.shape[0]
    components = field_vars + 1
    block_cells = packed_counts.shape[2]
    own_cells = src_depth.shape[0]
    own_tiles = own_cells // block_cells
    pair_slots = pair_source.shape[0]
    offset_count = 2 * REACH + 1
    capacity = max(2, 2 * pair_slots // offset_count)
    own_field = lax.all_to_all(src_field, "narrow", split_axis=2, concat_axis=1, tiled=True)
    levels = own_field.shape[1]
    part_levels = levels // narrow_size
    level_ids = jnp.arange(levels, dtype=jnp.int32)
    wet_levels = level_ids[:, None] < src_depth[None, :]
    masked = jnp.where(wet_levels[None, :, :], own_field, jnp.zeros_like(own_field))
    stacked = jnp.concatenate(
        [jnp.transpose(masked, (1, 0, 2)), wet_levels.astype(jnp.bfloat16)[:, None, :]], axis=1
    )
    by_tile = jnp.transpose(stacked.reshape(levels * components, own_tiles, block_cells), (1, 0, 2))
    picked = jnp.take(by_tile, pair_source, axis=0)
    weight = (unpack_counts(packed_counts).astype(jnp.float32) / DENOM).astype(jnp.bfloat16)
    pair_terms = lax.dot_general(
        picked, weight, (((2,), (2,)), ((0,), (0,))), preferred_element_type=jnp.float32
    )
    pair_terms = pair_terms.astype(jnp.bfloat16)
    is_live = jnp.arange(pair_slots, dtype=jnp.int32) < pair_count[0]
    wide_index = lax.axis_index("wide")
    destination = pair_home // TB_DEV
    local_block = pair_home % TB_DEV
    offset_index = (destination - wide_index + REACH + wide_size) % wide_size
    bound_for = (
        (offset_index[:, None] == jnp.arange(offset_count, dtype=jnp.int32)[None, :])
        & is_live[:, None]
    ).astype(jnp.int32)
    before = jnp.cumsum(bound_for, axis=0) - bound_for
    position = jnp.sum(before * bound_for, axis=1)
    slot_index = jnp.where(is_live, offset_index * capacity + position, offset_count * capacity)
    outgoing = (
        jnp.zeros((offset_count * capacity, levels * components, block_cells), jnp.bfloat16)
        .at[slot_index]
        .set(pair_terms, mode="drop")
    )
    targets = (
        jnp.full((offset_count * capacity,), TB_DEV, jnp.int32)
        .at[slot_index]
        .set(local_block, mode="drop")
    )
    outgoing = outgoing.reshape(offset_count, capacity, levels, components, block_cells)
    targets = targets.reshape(offset_count, capacity)
    shift_list = [shift_by for shift_by in range(-REACH, REACH + 1) if shift_by != 0]
    partial_value = block_sums(targets[REACH], outgoing[REACH], TB_DEV)
    for shift_by in shift_list:
        moved_terms, moved_owners = passed_along(
            (outgoing[REACH + shift_by], targets[REACH + shift_by]), "wide", shift_by
        )
        partial_value = partial_value + block_sums(moved_owners, moved_terms, TB_DEV)
    block_totals = lax.psum_scatter(partial_value, "narrow", scatter_dimension=0, tiled=True)
    numerators = block_totals[:, :field_vars]
    wet_total = block_totals[:, field_vars]
    covered = wet_total > wet_limit
    safe_wet = jnp.where(covered, wet_total, jnp.ones_like(wet_total))
    result = jnp.where(covered[:, None], numerators / safe_wet[:, None], jnp.zeros_like(numerators))
    result = jnp.transpose(result, (1, 0, 2, 3)).reshape(
        field_vars, part_levels, TB_DEV * block_cells
    )
    return result.astype(jnp.bfloat16)


SELF, MATE, RELAY, AHEAD, BEHIND = range(5)
LOADS = 4
EARLY = 2
SKEW = 8
LAG = 2
DIRECT = 1
LAST_GROUPS = (4, 1, 1, 1, 1)
VMEM_LIMIT = 26 * 2**20


def remap_kernel(
    sizes,
    field_hbm,
    depth_hbm,
    packed_hbm,
    source_hbm,
    home_hbm,
    count,
    out_ref,
    field,
    depth,
    source,
    home,
    field_in,
    slot_own,
    slot_in,
    words,
    weight,
    wets,
    fields_at,
    terms,
    select,
    cross_out,
    cross_in,
    own_terms,
    self_sum,
    sums_out,
    mate_in,
    far_in,
    across_in,
    inverse,
    staged,
    ready,
    load_sems,
    small_sems,
    entry_sems,
    sent_sems,
    cross_sems,
    mate_sems,
    far_sems,
    across_sems,
):
    wide_size, fields, levels, tiles, cells, pairs = sizes
    planes = (fields + 1) * levels
    pitch = pairs + SKEW
    f32, bf16, i32 = jnp.float32, jnp.bfloat16, jnp.int32
    w = lax.axis_index("wide")
    n = lax.axis_index("narrow")
    other = 1 - n
    sign = 1 - 2 * lax.rem(w, 2)
    mate = w + sign
    across = lax.rem(w - sign + wide_size, wide_size)
    ahead = lax.rem(w + 2 * sign + wide_size, wide_size)
    behind = lax.rem(w - 2 * sign + wide_size, wide_size)

    def signal(sem, place):
        pl.semaphore_signal(sem, inc=1, device_id=place, device_id_type=pl.DeviceIdType.MESH)

    barrier = pltpu.get_barrier_semaphore()
    signal(barrier, (w, other))
    signal(barrier, (mate, n))
    far_peers = ((ahead, 0, 1), (behind, 1, 0), (across, 2, 2))
    for far, _, _ in far_peers:

        @pl.when(far > w)
        def _():
            signal(barrier, (far, n))

    small = []
    for i, (src, dst) in enumerate(
        (
            (field_hbm, field),
            (home_hbm, home),
            (depth_hbm, depth),
            (source_hbm, source),
        )
    ):
        load = pltpu.make_async_copy(src, dst, small_sems.at[i])
        load.start()
        small.append(load)
    per_load = pairs // LOADS
    loads = []
    for i in range(LOADS):
        span = pl.ds(i * per_load, per_load)
        load = pltpu.make_async_copy(packed_hbm.at[span], words.at[span], load_sems.at[i])
        load.start()
        loads.append(load)

    def remote(src, dst, sent, received, place):
        return pltpu.make_async_remote_copy(
            src_ref=src,
            dst_ref=dst,
            send_sem=sent,
            recv_sem=received,
            device_id=place,
            device_id_type=pl.DeviceIdType.MESH,
        )

    own_cells = tiles * cells
    theirs = pl.ds(pl.multiple_of(other * own_cells, own_cells), own_cells)
    pl.semaphore_wait(barrier, 2 + sum((far < w).astype(i32) for far, _, _ in far_peers))
    for far, _, i in far_peers:

        @pl.when(far < w)
        def _():
            signal(ready.at[i], (far, n))

    small[0].wait()
    entry = [
        remote(field.at[:, :, theirs], field_in, entry_sems.at[0], entry_sems.at[1], (w, other))
    ]
    entry[0].start()
    small[1].wait()
    wide_home = lax.div(home[...], TB_DEV)
    offset = lax.rem(wide_home - w + REACH + wide_size, wide_size) - REACH
    toward = offset * sign
    slot = jnp.where(toward > 0, 2 * toward - 1, -2 * toward)
    is_live = lax.broadcasted_iota(i32, (1, pairs), 1) < count[0]
    slot_own[...] = jnp.where(is_live, slot * TB_DEV + home[...] - wide_home * TB_DEV, -1)
    entry.append(remote(slot_own, slot_in, entry_sems.at[2], entry_sems.at[3], (w, other)))
    entry[1].start()

    small[2].wait()
    rows = lax.broadcasted_iota(i32, (2 * levels, cells), 0)
    level_of = jnp.where(rows < levels, rows + other * levels, rows - levels + n * levels)
    for tile in range(tiles):
        wet = level_of < depth[pl.ds(tile, 1), :]
        wets[tile] = jnp.where(wet, 1.0, 0.0).astype(bf16)

    half = cells // 2

    def unpack(first):
        for u in range(per_load):
            p = first + u
            word = words[p]
            lanes = pl.ds((u % 2) * cells, cells)
            low = (word & 65535).astype(f32).astype(bf16)
            high = (word >> 16).astype(f32).astype(bf16)
            weight[(first + u) // 2, pl.ds(0, half), lanes] = low
            weight[(first + u) // 2, pl.ds(half, half), lanes] = high

    def multiply(values_of, count, base, first):
        zero = jnp.zeros((count, cells), bf16)
        for u in range(0, per_load, 2):
            p = first + u
            left = jnp.concatenate([values_of[source[p]], zero], axis=1)
            right = jnp.concatenate([zero, values_of[source[p + 1]]], axis=1)
            term = lax.dot_general(
                jnp.concatenate([left, right], axis=0),
                weight[p // 2],
                (((1,), (1,)), ((), ())),
                preferred_element_type=f32,
            )
            terms[pl.ds(base * pitch + p, count, stride=pitch), :] = term[:count]
            terms[pl.ds(base * pitch + p + 1, count, stride=pitch), :] = term[count:]

    def rounded(row, start, count):
        return terms[pl.ds(row * pitch + start, count), :].astype(bf16)

    small[3].wait()
    loads[0].wait()
    unpack(0)
    sent_cross, sent_mate, sent_ahead, sent_behind = (sent_sems.at[i] for i in range(4))
    some = pl.ds(0, EARLY)
    for batch in range(LOADS):
        first = batch * per_load
        if batch + 1 < LOADS:
            loads[batch + 1].wait()
            unpack(first + per_load)
        multiply(wets, 2 * levels, 0, first)
        span = pl.ds(first, per_load)
        for q in range(EARLY):
            cross_out[q, span, :] = rounded(q, first, per_load)
        remote(
            cross_out.at[some, span, :], cross_in.at[some, span, :],
            sent_cross, cross_sems.at[0], (w, other),
        ).start()

    def cross(some, i):
        return remote(
            cross_out.at[some], cross_in.at[some], sent_cross, cross_sems.at[i], (w, other)
        )

    def send_terms(q):
        cross_out[q] = rounded(q if q < levels else q + levels, 0, pairs)
        cross(pl.ds(q, 1), q - EARLY + 1).start()

    for q in range(EARLY, levels):
        send_terms(q)

    level_ids = lax.broadcasted_iota(i32, (levels, cells), 0)

    def stack(side, group, read):
        for tile in range(tiles):
            wet = level_ids + group * levels < depth[pl.ds(tile, 1), :]
            values = [jnp.where(wet, read(k, tile).astype(f32), 0.0) for k in range(fields)]
            fields_at[tile, pl.ds(side * fields * levels, fields * levels), :] = (
                jnp.concatenate(values, axis=0).astype(bf16)
            )

    own_start = n * own_cells
    stack(
        1,
        n,
        lambda k, tile: field[k, :, pl.ds(pl.multiple_of(own_start + tile * cells, cells), cells)],
    )
    for q in range(levels):
        own_terms[q] = rounded(q + levels, 0, pairs)

    entry[1].wait()
    slots = lax.broadcasted_iota(i32, (5 * TB_DEV, pairs), 0)
    select[:, pl.ds(0, pairs)] = jnp.where(slots == slot_own[...], 1.0, 0.0).astype(bf16)
    select[:, pl.ds(pairs, pairs)] = jnp.where(slots == slot_in[...], 1.0, 0.0).astype(bf16)

    for far, i, _ in far_peers:

        @pl.when(far > w)
        def _():
            pl.semaphore_wait(ready.at[i], 1)

    groups = (planes - sum(LAST_GROUPS),) + LAST_GROUPS
    group_of = [g for g, size in enumerate(groups) for _ in range(size)]

    first_direct = planes - DIRECT

    def to_mate(q):
        slots_here = pl.ds(0, 2 if q < first_direct else 1)
        src, dst = sums_out.at[q, slots_here], mate_in.at[q, slots_here]
        return remote(src, dst, sent_mate, mate_sems.at[q], (mate, n))

    direct = sums_out.at[pl.ds(first_direct, DIRECT), RELAY - 1]
    to_across = remote(direct, across_in, sent_mate, across_sems.at[0], (across, n))

    def to_ahead(some, i):
        src, dst = sums_out.at[some, pl.ds(AHEAD - 1, 1)], far_in.at[some, pl.ds(0, 1)]
        return remote(src, dst, sent_ahead, far_sems.at[i], (ahead, n))

    def to_behind(some, i):
        src, dst = sums_out.at[some, pl.ds(BEHIND - 1, 1)], far_in.at[some, pl.ds(1, 1)]
        return remote(src, dst, sent_behind, far_sems.at[i], (behind, n))

    def pass_on(q):
        to_mate(q).wait_recv()
        sums_out[q, AHEAD - 1] = (
            sums_out[q, AHEAD - 1].astype(f32) + mate_in[q, RELAY - 1].astype(f32)
        ).astype(bf16)
        to_ahead(pl.ds(q, 1), group_of[q]).start()

    def add_up(q):
        if q == 0:
            cross(some, 0).wait_recv()
        if q >= EARLY:
            cross(pl.ds(q, 1), q - EARLY + 1).wait_recv()
        pair_values = jnp.concatenate([own_terms[q], cross_in[q]], axis=0)
        sums = jnp.dot(select[...], pair_values, preferred_element_type=f32)
        self_sum[q] = sums[:TB_DEV]
        for slot in (MATE, RELAY, AHEAD, BEHIND):
            sums_out[q, slot - 1] = sums[slot * TB_DEV : (slot + 1) * TB_DEV].astype(bf16)
        if q >= first_direct:
            to_ahead(pl.ds(q, 1), group_of[q]).start()
        if q == planes - 1:
            to_across.start()
        to_mate(q).start()
        to_behind(pl.ds(q, 1), group_of[q]).start()
        if LAG <= q < first_direct + LAG:
            pass_on(q - LAG)

    entry[0].wait()
    stack(0, other, lambda k, tile: field_in[k, :, pl.ds(tile * cells, cells)])
    for batch in range(LOADS):
        multiply(fields_at, 2 * fields * levels, 2 * levels, batch * per_load)
    for q in range(levels, planes):
        send_terms(q)
    for q in range(levels, planes):
        own_terms[q] = rounded(q + levels + fields * levels, 0, pairs)
    for q in range(planes):
        add_up(q)
    for q in range(planes - LAG, first_direct):
        pass_on(q)

    for q in range(planes):
        if q == groups[0]:
            cross(pl.ds(0, planes), 0).wait_send()
        if q == planes - 1:
            for copy in (to_behind, to_ahead):
                copy(pl.ds(0, planes), 0).wait_send()
            remote(
                sums_out.at[:, pl.ds(0, 2)], mate_in, sent_mate, mate_sems.at[0], (mate, n)
            ).wait_send()
        if q == 0 or group_of[q] != group_of[q - 1]:
            arrived = far_in.at[pl.ds(q, groups[group_of[q]])]
            remote(arrived, arrived, sent_ahead, far_sems.at[group_of[q]], (ahead, n)).wait_recv()
        if q >= first_direct:
            to_mate(q).wait_recv()
        if q == first_direct:
            to_across.wait_recv()
        total = (
            self_sum[q]
            + mate_in[q, MATE - 1].astype(f32)
            + far_in[q, 0].astype(f32)
            + far_in[q, 1].astype(f32)
        )
        if q >= first_direct:
            total = total + across_in[q - first_direct].astype(f32)
        if q < levels:
            covered = total > wet_limit * DENOM
            inverse[q] = jnp.where(covered, 1.0 / jnp.where(covered, total, 1.0), 0.0)
            continue
        k, level = divmod(q - levels, levels)
        staged[pl.ds(level, TB_DEV, stride=levels), :] = total * inverse[level]
        if level == levels - 1:
            for block in range(TB_DEV):
                out_ref[k, :, pl.ds(block * cells, cells)] = staged[
                    pl.ds(block * levels, levels), :
                ].astype(out_ref.dtype)


def by_kernel(src_field, src_depth, packed_counts, pair_source, pair_home, pair_count):
    wide_size = lax.axis_size("wide")
    fields, levels, _ = src_field.shape
    pairs, _, cells = packed_counts.shape
    tiles = src_depth.shape[0] // cells
    planes = (fields + 1) * levels
    sizes = (wide_size, fields, levels, tiles, cells, pairs)
    hbm = pl.BlockSpec(memory_space=pltpu.HBM)
    bf16, f32, i32 = jnp.bfloat16, jnp.float32, jnp.int32
    terms_shape = (planes, pairs, cells)
    block_shape = (TB_DEV, cells)
    operands = (
        src_field,
        src_depth.reshape(tiles, cells),
        packed_counts,
        pair_source,
        pair_home.reshape(1, pairs),
    )
    return pl.pallas_call(
        functools.partial(remap_kernel, sizes),
        out_shape=jax.ShapeDtypeStruct((fields, levels, TB_DEV * cells), bf16),
        in_specs=[hbm] * len(operands) + [pl.BlockSpec(memory_space=pltpu.SMEM)],
        out_specs=pl.BlockSpec(memory_space=pltpu.VMEM),
        scratch_shapes=[
            pltpu.VMEM(src_field.shape, bf16),
            pltpu.VMEM((tiles, cells), i32),
            pltpu.SMEM((pairs,), i32),
            pltpu.VMEM((1, pairs), i32),
            pltpu.VMEM((fields, levels, tiles * cells), bf16),
            pltpu.VMEM((1, pairs), i32),
            pltpu.VMEM((1, pairs), i32),
            pltpu.VMEM((pairs, cells // 2, cells), i32),
            pltpu.VMEM((pairs // 2, cells, 2 * cells), bf16),
            pltpu.VMEM((tiles, 2 * levels, cells), bf16),
            pltpu.VMEM((tiles, 2 * fields * levels, cells), bf16),
            pltpu.VMEM((2 * planes * (pairs + SKEW), cells), f32),
            pltpu.VMEM((5 * TB_DEV, 2 * pairs), bf16),
            pltpu.VMEM(terms_shape, bf16),
            pltpu.VMEM(terms_shape, bf16),
            pltpu.VMEM(terms_shape, bf16),
            pltpu.VMEM((planes,) + block_shape, f32),
            pltpu.VMEM((planes, 4) + block_shape, bf16),
            pltpu.VMEM((planes, 2) + block_shape, bf16),
            pltpu.VMEM((planes, 2) + block_shape, bf16),
            pltpu.VMEM((DIRECT,) + block_shape, bf16),
            pltpu.VMEM((levels,) + block_shape, f32),
            pltpu.VMEM((TB_DEV * levels, cells), f32),
            pltpu.SemaphoreType.REGULAR((3,)),
            pltpu.SemaphoreType.DMA((LOADS,)),
            pltpu.SemaphoreType.DMA((4,)),
            pltpu.SemaphoreType.DMA((4,)),
            pltpu.SemaphoreType.DMA((4,)),
            pltpu.SemaphoreType.DMA((planes - EARLY + 1,)),
            pltpu.SemaphoreType.DMA((planes,)),
            pltpu.SemaphoreType.DMA((1 + len(LAST_GROUPS),)),
            pltpu.SemaphoreType.DMA((1,)),
        ],
        compiler_params=pltpu.CompilerParams(
            collective_id=0, has_side_effects=True, vmem_limit_bytes=VMEM_LIMIT
        ),
        name="remap",
    )(
        *(pltpu.with_memory_space_constraint(x, pltpu.HBM) for x in operands),
        pair_count,
    )


def solution(mesh):
    placed = (
        P(None, "narrow", "wide"),
        P(("wide", "narrow")),
        P(("wide", "narrow"), None, None),
        P(("wide", "narrow")),
        P(("wide", "narrow")),
        P(("wide", "narrow")),
    )
    paired = mesh.shape["narrow"] == 2 and mesh.shape["wide"] % 2 == 0
    fits = paired and mesh.shape["wide"] > 2 * REACH and REACH == 2
    return jax.shard_map(
        by_kernel if fits else by_collectives,
        mesh=mesh,
        in_specs=placed,
        out_specs=P(None, "narrow", "wide"),
        check_vma=False,
    )
```

```python
import functools

import jax
import jax.numpy as jnp
from jax import lax
from jax.experimental import pallas as pl
from jax.experimental.pallas import tpu as pltpu
from jax.sharding import PartitionSpec as P

DENOM = 256
REACH = 2
TB_DEV = 64


wet_limit = 0.001


def passed_along(block, axis, distance):
    devices = range(lax.axis_size(axis))
    route = [((i - distance) % len(devices), i) for i in devices]
    return lax.ppermute(block, axis, route)


def unpack_counts(packed_words):
    return jnp.concatenate([packed_words % 65536, packed_words // 65536], axis=-2)


def block_sums(targets, received, block_count):
    owners = jnp.arange(block_count, dtype=jnp.int32)
    select = (targets[:, None] == owners[None, :]).astype(jnp.bfloat16)
    return jnp.einsum("rq,rlcb->lcqb", select, received, preferred_element_type=jnp.float32)


def by_collectives(src_field, src_depth, packed_counts, pair_source, pair_home, pair_count):
    narrow_size = lax.axis_size("narrow")
    wide_size = lax.axis_size("wide")
    field_vars = src_field.shape[0]
    components = field_vars + 1
    block_cells = packed_counts.shape[2]
    own_cells = src_depth.shape[0]
    own_tiles = own_cells // block_cells
    pair_slots = pair_source.shape[0]
    offset_count = 2 * REACH + 1
    capacity = max(2, 2 * pair_slots // offset_count)
    own_field = lax.all_to_all(src_field, "narrow", split_axis=2, concat_axis=1, tiled=True)
    levels = own_field.shape[1]
    part_levels = levels // narrow_size
    level_ids = jnp.arange(levels, dtype=jnp.int32)
    wet_levels = level_ids[:, None] < src_depth[None, :]
    masked = jnp.where(wet_levels[None, :, :], own_field, jnp.zeros_like(own_field))
    stacked = jnp.concatenate(
        [jnp.transpose(masked, (1, 0, 2)), wet_levels.astype(jnp.bfloat16)[:, None, :]], axis=1
    )
    by_tile = jnp.transpose(stacked.reshape(levels * components, own_tiles, block_cells), (1, 0, 2))
    picked = jnp.take(by_tile, pair_source, axis=0)
    weight = (unpack_counts(packed_counts).astype(jnp.float32) / DENOM).astype(jnp.bfloat16)
    pair_terms = lax.dot_general(
        picked, weight, (((2,), (2,)), ((0,), (0,))), preferred_element_type=jnp.float32
    )
    pair_terms = pair_terms.astype(jnp.bfloat16)
    is_live = jnp.arange(pair_slots, dtype=jnp.int32) < pair_count[0]
    wide_index = lax.axis_index("wide")
    destination = pair_home // TB_DEV
    local_block = pair_home % TB_DEV
    offset_index = (destination - wide_index + REACH + wide_size) % wide_size
    bound_for = (
        (offset_index[:, None] == jnp.arange(offset_count, dtype=jnp.int32)[None, :])
        & is_live[:, None]
    ).astype(jnp.int32)
    before = jnp.cumsum(bound_for, axis=0) - bound_for
    position = jnp.sum(before * bound_for, axis=1)
    slot_index = jnp.where(is_live, offset_index * capacity + position, offset_count * capacity)
    outgoing = (
        jnp.zeros((offset_count * capacity, levels * components, block_cells), jnp.bfloat16)
        .at[slot_index]
        .set(pair_terms, mode="drop")
    )
    targets = (
        jnp.full((offset_count * capacity,), TB_DEV, jnp.int32)
        .at[slot_index]
        .set(local_block, mode="drop")
    )
    outgoing = outgoing.reshape(offset_count, capacity, levels, components, block_cells)
    targets = targets.reshape(offset_count, capacity)
    shift_list = [shift_by for shift_by in range(-REACH, REACH + 1) if shift_by != 0]
    partial_value = block_sums(targets[REACH], outgoing[REACH], TB_DEV)
    for shift_by in shift_list:
        moved_terms, moved_owners = passed_along(
            (outgoing[REACH + shift_by], targets[REACH + shift_by]), "wide", shift_by
        )
        partial_value = partial_value + block_sums(moved_owners, moved_terms, TB_DEV)
    block_totals = lax.psum_scatter(partial_value, "narrow", scatter_dimension=0, tiled=True)
    numerators = block_totals[:, :field_vars]
    wet_total = block_totals[:, field_vars]
    covered = wet_total > wet_limit
    safe_wet = jnp.where(covered, wet_total, jnp.ones_like(wet_total))
    result = jnp.where(covered[:, None], numerators / safe_wet[:, None], jnp.zeros_like(numerators))
    result = jnp.transpose(result, (1, 0, 2, 3)).reshape(
        field_vars, part_levels, TB_DEV * block_cells
    )
    return result.astype(jnp.bfloat16)


SELF, MATE, RELAY, AHEAD, BEHIND = range(5)
LOADS = 4
EARLY = 2
SKEW = 8
LAG = 2
DIRECT = 1
RING = 4 + 2 * LAG
LAST_GROUPS = (4, 1, 1, 1, 1)
VMEM_LIMIT = 26 * 2**20


def remap_kernel(
    sizes,
    field_hbm,
    depth_hbm,
    packed_hbm,
    source_hbm,
    home_hbm,
    count,
    out_ref,
    field,
    depth,
    source,
    home,
    field_in,
    slot_own,
    slot_in,
    words,
    weight,
    wets,
    fields_at,
    terms,
    select,
    cross_out,
    cross_in,
    own_terms,
    self_sum,
    sums_out,
    mate_in,
    far_in,
    across_in,
    inverse,
    staged,
    ready,
    load_sems,
    small_sems,
    entry_sems,
    sent_sems,
    cross_sems,
    mate_sems,
    far_sems,
    across_sems,
):
    wide_size, fields, levels, tiles, cells, pairs = sizes
    planes = (fields + 1) * levels
    pitch = pairs + SKEW
    f32, bf16, i32 = jnp.float32, jnp.bfloat16, jnp.int32
    w = lax.axis_index("wide")
    n = lax.axis_index("narrow")
    other = 1 - n
    sign = 1 - 2 * lax.rem(w, 2)
    mate = w + sign
    across = lax.rem(w - sign + wide_size, wide_size)
    ahead = lax.rem(w + 2 * sign + wide_size, wide_size)
    behind = lax.rem(w - 2 * sign + wide_size, wide_size)

    def signal(sem, place):
        pl.semaphore_signal(sem, inc=1, device_id=place, device_id_type=pl.DeviceIdType.MESH)

    barrier = pltpu.get_barrier_semaphore()
    signal(barrier, (w, other))
    signal(barrier, (mate, n))
    far_peers = ((ahead, 0, 1), (behind, 1, 0), (across, 2, 2))
    for far, _, _ in far_peers:

        @pl.when(far > w)
        def _():
            signal(barrier, (far, n))

    small = []
    for i, (src, dst) in enumerate(
        (
            (field_hbm, field),
            (home_hbm, home),
            (depth_hbm, depth),
            (source_hbm, source),
        )
    ):
        load = pltpu.make_async_copy(src, dst, small_sems.at[i])
        load.start()
        small.append(load)
    per_load = pairs // LOADS
    loads = []
    for i in range(LOADS):
        span = pl.ds(i * per_load, per_load)
        load = pltpu.make_async_copy(packed_hbm.at[span], words.at[span], load_sems.at[i])
        load.start()
        loads.append(load)

    def remote(src, dst, sent, received, place):
        return pltpu.make_async_remote_copy(
            src_ref=src,
            dst_ref=dst,
            send_sem=sent,
            recv_sem=received,
            device_id=place,
            device_id_type=pl.DeviceIdType.MESH,
        )

    own_cells = tiles * cells
    theirs = pl.ds(pl.multiple_of(other * own_cells, own_cells), own_cells)
    pl.semaphore_wait(barrier, 2 + sum((far < w).astype(i32) for far, _, _ in far_peers))
    for far, _, i in far_peers:

        @pl.when(far < w)
        def _():
            signal(ready.at[i], (far, n))

    small[0].wait()
    entry = [
        remote(field.at[:, :, theirs], field_in, entry_sems.at[0], entry_sems.at[1], (w, other))
    ]
    entry[0].start()
    small[1].wait()
    wide_home = lax.div(home[...], TB_DEV)
    offset = lax.rem(wide_home - w + REACH + wide_size, wide_size) - REACH
    toward = offset * sign
    slot = jnp.where(toward > 0, 2 * toward - 1, -2 * toward)
    is_live = lax.broadcasted_iota(i32, (1, pairs), 1) < count[0]
    slot_own[...] = jnp.where(is_live, slot * TB_DEV + home[...] - wide_home * TB_DEV, -1)
    entry.append(remote(slot_own, slot_in, entry_sems.at[2], entry_sems.at[3], (w, other)))
    entry[1].start()

    small[2].wait()
    rows = lax.broadcasted_iota(i32, (2 * levels, cells), 0)
    level_of = jnp.where(rows < levels, rows + other * levels, rows - levels + n * levels)
    for tile in range(tiles):
        wet = level_of < depth[pl.ds(tile, 1), :]
        wets[tile] = jnp.where(wet, 1.0, 0.0).astype(bf16)

    half = cells // 2

    def unpack(first):
        for u in range(per_load):
            p = first + u
            word = words[p]
            lanes = pl.ds((u % 2) * cells, cells)
            low = (word & 65535).astype(f32).astype(bf16)
            high = (word >> 16).astype(f32).astype(bf16)
            weight[(first + u) // 2, pl.ds(0, half), lanes] = low
            weight[(first + u) // 2, pl.ds(half, half), lanes] = high

    def multiply(values_of, count, base, first):
        zero = jnp.zeros((count, cells), bf16)
        for u in range(0, per_load, 2):
            p = first + u
            left = jnp.concatenate([values_of[source[p]], zero], axis=1)
            right = jnp.concatenate([zero, values_of[source[p + 1]]], axis=1)
            term = lax.dot_general(
                jnp.concatenate([left, right], axis=0),
                weight[p // 2],
                (((1,), (1,)), ((), ())),
                preferred_element_type=f32,
            )
            terms[pl.ds(base * pitch + p, count, stride=pitch), :] = term[:count]
            terms[pl.ds(base * pitch + p + 1, count, stride=pitch), :] = term[count:]

    def rounded(row, start, count):
        return terms[pl.ds(row * pitch + start, count), :].astype(bf16)

    small[3].wait()
    loads[0].wait()
    unpack(0)
    sent_cross, sent_sums = sent_sems.at[0], sent_sems.at[1]
    some = pl.ds(0, EARLY)
    for batch in range(LOADS):
        first = batch * per_load
        if batch + 1 < LOADS:
            loads[batch + 1].wait()
            unpack(first + per_load)
        multiply(wets, 2 * levels, 0, first)
        span = pl.ds(first, per_load)
        for q in range(EARLY):
            cross_out[q, span, :] = rounded(q, first, per_load)
        remote(
            cross_out.at[some, span, :], cross_in.at[some, span, :],
            sent_cross, cross_sems.at[0], (w, other),
        ).start()

    def cross(some, i):
        return remote(
            cross_out.at[some], cross_in.at[some], sent_cross, cross_sems.at[i], (w, other)
        )

    def send_terms(q):
        cross_out[q] = rounded(q if q < levels else q + levels, 0, pairs)
        cross(pl.ds(q, 1), q - EARLY + 1).start()

    for q in range(EARLY, levels):
        send_terms(q)

    level_ids = lax.broadcasted_iota(i32, (levels, cells), 0)

    def stack(side, group, read):
        for tile in range(tiles):
            wet = level_ids + group * levels < depth[pl.ds(tile, 1), :]
            values = [jnp.where(wet, read(k, tile).astype(f32), 0.0) for k in range(fields)]
            fields_at[tile, pl.ds(side * fields * levels, fields * levels), :] = (
                jnp.concatenate(values, axis=0).astype(bf16)
            )

    own_start = n * own_cells
    stack(
        1,
        n,
        lambda k, tile: field[k, :, pl.ds(pl.multiple_of(own_start + tile * cells, cells), cells)],
    )
    for q in range(levels):
        own_terms[q] = rounded(q + levels, 0, pairs)

    entry[1].wait()
    slots = lax.broadcasted_iota(i32, (5 * TB_DEV, pairs), 0)
    select[:, pl.ds(0, pairs)] = jnp.where(slots == slot_own[...], 1.0, 0.0).astype(bf16)
    select[:, pl.ds(pairs, pairs)] = jnp.where(slots == slot_in[...], 1.0, 0.0).astype(bf16)

    for far, i, _ in far_peers:

        @pl.when(far > w)
        def _():
            pl.semaphore_wait(ready.at[i], 1)

    groups = (planes - sum(LAST_GROUPS),) + LAST_GROUPS
    group_of = [g for g, size in enumerate(groups) for _ in range(size)]

    first_direct = planes - DIRECT

    def to_mate(q):
        slots_here = pl.ds(0, 2 if q < first_direct else 1)
        src, dst = sums_out.at[q, slots_here], mate_in.at[q, slots_here]
        return remote(src, dst, sent_sums, mate_sems.at[q % RING], (mate, n))

    direct = sums_out.at[pl.ds(first_direct, DIRECT), RELAY - 1]
    to_across = remote(direct, across_in, sent_sums, across_sems.at[0], (across, n))

    def to_ahead(some, i):
        src, dst = sums_out.at[some, pl.ds(AHEAD - 1, 1)], far_in.at[some, pl.ds(0, 1)]
        return remote(src, dst, sent_sums, far_sems.at[i], (ahead, n))

    def to_behind(some, i):
        src, dst = sums_out.at[some, pl.ds(BEHIND - 1, 1)], far_in.at[some, pl.ds(1, 1)]
        return remote(src, dst, sent_sums, far_sems.at[i], (behind, n))

    def pass_on(q):
        to_mate(q).wait_recv()
        sums_out[q, AHEAD - 1] = (
            sums_out[q, AHEAD - 1].astype(f32) + mate_in[q, RELAY - 1].astype(f32)
        ).astype(bf16)
        to_ahead(pl.ds(q, 1), group_of[q]).start()

    def add_up(q):
        if q == 0:
            cross(some, 0).wait_recv()
        if q >= EARLY:
            cross(pl.ds(q, 1), q - EARLY + 1).wait_recv()
        pair_values = jnp.concatenate([own_terms[q], cross_in[q]], axis=0)
        sums = jnp.dot(select[...], pair_values, preferred_element_type=f32)
        self_sum[q] = sums[:TB_DEV]
        for slot in (MATE, RELAY, AHEAD, BEHIND):
            sums_out[q, slot - 1] = sums[slot * TB_DEV : (slot + 1) * TB_DEV].astype(bf16)
        if q >= first_direct:
            to_ahead(pl.ds(q, 1), group_of[q]).start()
        if q == planes - 1:
            to_across.start()
        to_mate(q).start()
        to_behind(pl.ds(q, 1), group_of[q]).start()
        if LAG <= q < first_direct + LAG:
            pass_on(q - LAG)

    entry[0].wait()
    stack(0, other, lambda k, tile: field_in[k, :, pl.ds(tile * cells, cells)])
    for batch in range(LOADS):
        multiply(fields_at, 2 * fields * levels, 2 * levels, batch * per_load)
    for q in range(levels, planes):
        send_terms(q)
    for q in range(levels, planes):
        own_terms[q] = rounded(q + levels + fields * levels, 0, pairs)
    for q in range(planes):
        add_up(q)
    for q in range(planes - LAG, first_direct):
        pass_on(q)

    for q in range(planes):
        if q == groups[0]:
            cross(pl.ds(0, planes), 0).wait_send()
        if q == planes - 1:
            remote(sums_out, sums_out, sent_sums, mate_sems.at[0], (mate, n)).wait_send()
        if q == 0 or group_of[q] != group_of[q - 1]:
            arrived = far_in.at[pl.ds(q, groups[group_of[q]])]
            remote(arrived, arrived, sent_sums, far_sems.at[group_of[q]], (ahead, n)).wait_recv()
        if q >= first_direct:
            to_mate(q).wait_recv()
        if q == first_direct:
            to_across.wait_recv()
        total = (
            self_sum[q]
            + mate_in[q, MATE - 1].astype(f32)
            + far_in[q, 0].astype(f32)
            + far_in[q, 1].astype(f32)
        )
        if q >= first_direct:
            total = total + across_in[q - first_direct].astype(f32)
        if q < levels:
            covered = total > wet_limit * DENOM
            inverse[q] = jnp.where(covered, 1.0 / jnp.where(covered, total, 1.0), 0.0)
            continue
        k, level = divmod(q - levels, levels)
        staged[pl.ds(level, TB_DEV, stride=levels), :] = total * inverse[level]
        if level == levels - 1:
            for block in range(TB_DEV):
                out_ref[k, :, pl.ds(block * cells, cells)] = staged[
                    pl.ds(block * levels, levels), :
                ].astype(out_ref.dtype)


def by_kernel(src_field, src_depth, packed_counts, pair_source, pair_home, pair_count):
    wide_size = lax.axis_size("wide")
    fields, levels, _ = src_field.shape
    pairs, _, cells = packed_counts.shape
    tiles = src_depth.shape[0] // cells
    planes = (fields + 1) * levels
    sizes = (wide_size, fields, levels, tiles, cells, pairs)
    hbm = pl.BlockSpec(memory_space=pltpu.HBM)
    bf16, f32, i32 = jnp.bfloat16, jnp.float32, jnp.int32
    terms_shape = (planes, pairs, cells)
    block_shape = (TB_DEV, cells)
    operands = (
        src_field,
        src_depth.reshape(tiles, cells),
        packed_counts,
        pair_source,
        pair_home.reshape(1, pairs),
    )
    return pl.pallas_call(
        functools.partial(remap_kernel, sizes),
        out_shape=jax.ShapeDtypeStruct((fields, levels, TB_DEV * cells), bf16),
        in_specs=[hbm] * len(operands) + [pl.BlockSpec(memory_space=pltpu.SMEM)],
        out_specs=pl.BlockSpec(memory_space=pltpu.VMEM),
        scratch_shapes=[
            pltpu.VMEM(src_field.shape, bf16),
            pltpu.VMEM((tiles, cells), i32),
            pltpu.SMEM((pairs,), i32),
            pltpu.VMEM((1, pairs), i32),
            pltpu.VMEM((fields, levels, tiles * cells), bf16),
            pltpu.VMEM((1, pairs), i32),
            pltpu.VMEM((1, pairs), i32),
            pltpu.VMEM((pairs, cells // 2, cells), i32),
            pltpu.VMEM((pairs // 2, cells, 2 * cells), bf16),
            pltpu.VMEM((tiles, 2 * levels, cells), bf16),
            pltpu.VMEM((tiles, 2 * fields * levels, cells), bf16),
            pltpu.VMEM((2 * planes * (pairs + SKEW), cells), f32),
            pltpu.VMEM((5 * TB_DEV, 2 * pairs), bf16),
            pltpu.VMEM(terms_shape, bf16),
            pltpu.VMEM(terms_shape, bf16),
            pltpu.VMEM(terms_shape, bf16),
            pltpu.VMEM((planes,) + block_shape, f32),
            pltpu.VMEM((planes, 4) + block_shape, bf16),
            pltpu.VMEM((planes, 2) + block_shape, bf16),
            pltpu.VMEM((planes, 2) + block_shape, bf16),
            pltpu.VMEM((DIRECT,) + block_shape, bf16),
            pltpu.VMEM((levels,) + block_shape, f32),
            pltpu.VMEM((TB_DEV * levels, cells), f32),
            pltpu.SemaphoreType.REGULAR((3,)),
            pltpu.SemaphoreType.DMA((LOADS,)),
            pltpu.SemaphoreType.DMA((4,)),
            pltpu.SemaphoreType.DMA((4,)),
            pltpu.SemaphoreType.DMA((2,)),
            pltpu.SemaphoreType.DMA((planes - EARLY + 1,)),
            pltpu.SemaphoreType.DMA((RING,)),
            pltpu.SemaphoreType.DMA((1 + len(LAST_GROUPS),)),
            pltpu.SemaphoreType.DMA((1,)),
        ],
        compiler_params=pltpu.CompilerParams(
            collective_id=0, has_side_effects=True, vmem_limit_bytes=VMEM_LIMIT
        ),
        name="remap",
    )(
        *(pltpu.with_memory_space_constraint(x, pltpu.HBM) for x in operands),
        pair_count,
    )


def solution(mesh):
    placed = (
        P(None, "narrow", "wide"),
        P(("wide", "narrow")),
        P(("wide", "narrow"), None, None),
        P(("wide", "narrow")),
        P(("wide", "narrow")),
        P(("wide", "narrow")),
    )
    paired = mesh.shape["narrow"] == 2 and mesh.shape["wide"] % 2 == 0
    fits = paired and mesh.shape["wide"] > 2 * REACH and REACH == 2
    return jax.shard_map(
        by_kernel if fits else by_collectives,
        mesh=mesh,
        in_specs=placed,
        out_specs=P(None, "narrow", "wide"),
        check_vma=False,
    )
```
